128 devices in a mesh: dp: 16 (over z, y), sp: 8 (over x, core).
Axes of the slice: x: 4, y: 4, z: 4, core: 2. Of those that a mesh axis runs over, the one named last changes fastest.
Arguments:
- tokens: bfloat16 [16, 2048, 2048], P('dp', 'sp')
- grad_out: bfloat16 [16, 2048, 2048], P('dp', 'sp')
- norm_attn: bfloat16 [2048], replicated
- w_query: bfloat16 [2048, 2048], replicated
- w_key: bfloat16 [2048, 1024], replicated
- w_value: bfloat16 [2048, 1024], replicated
- w_out: bfloat16 [2048, 2048], replicated
- norm_mlp: bfloat16 [2048], replicated
- w_gate: bfloat16 [2048, 6144], replicated
- w_up: bfloat16 [2048, 6144], replicated
- w_down: bfloat16 [6144, 2048], replicated
Outputs:
- output 1: bfloat16 [16, 2048, 2048], P('dp', 'sp')
- output 2: float32 [2048], replicated
- output 3: float32 [2048, 2048], replicated
- output 4: float32 [2048, 1024], replicated
- output 5: float32 [2048, 1024], replicated
- output 6: float32 [2048, 2048], replicated
- output 7: float32 [2048], replicated
- output 8: float32 [2048, 6144], replicated
- output 9: float32 [2048, 6144], replicated
- output 10: float32 [6144, 2048], replicated
All inputs are finite; a program needn't handle non-finite values.
Results may differ from the reference program's by a relative error of at most 0.02.
Values are sent between devices in bfloat16 or wider.
A program may use at most 1.25 GiB of HBM per device.

```python
import jax
import jax.numpy as jnp
from jax import lax

BATCH_SIZE = 16
SEQ_LEN = 2048
MODEL_DIM = 2048
Q_HEADS = 16
KV_HEADS = 8
HEAD_DIM = 128
FF_DIM = 6144
NORM_EPS = 1.0e-5
ROPE_BASE = 1.0e6
SCORE_CAP = 2 ** 24


def setup_inputs(seed: int = 0) -> dict:
    key_list = jax.random.split(jax.random.key(seed), 11)
    q_width = Q_HEADS * HEAD_DIM
    kv_width = KV_HEADS * HEAD_DIM
    seq_shape = (BATCH_SIZE, SEQ_LEN, MODEL_DIM)
    qk_std = 1.6 * MODEL_DIM ** -0.5

    def normal_draw(rng_key, arr_shape, std_scale, center):
        return (jax.random.normal(rng_key, arr_shape, jnp.float32) * std_scale + center).astype(jnp.bfloat16)

    return {
        "tokens": normal_draw(key_list[0], seq_shape, 1.0, 0.0),
        "grad_out": normal_draw(key_list[1], seq_shape, 1.0, 0.0),
        "norm_attn": normal_draw(key_list[2], (MODEL_DIM,), 0.3, 1.0),
        "w_query": normal_draw(key_list[3], (MODEL_DIM, q_width), qk_std, 0.0),
        "w_key": normal_draw(key_list[4], (MODEL_DIM, kv_width), qk_std, 0.0),
        "w_value": normal_draw(key_list[5], (MODEL_DIM, kv_width), MODEL_DIM ** -0.5, 0.0),
        "w_out": normal_draw(key_list[6], (q_width, MODEL_DIM), q_width ** -0.5, 0.0),
        "norm_mlp": normal_draw(key_list[7], (MODEL_DIM,), 0.3, 1.0),
        "w_gate": normal_draw(key_list[8], (MODEL_DIM, FF_DIM), MODEL_DIM ** -0.5, 0.0),
        "w_up": normal_draw(key_list[9], (MODEL_DIM, FF_DIM), MODEL_DIM ** -0.5, 0.0),
        "w_down": normal_draw(key_list[10], (FF_DIM, MODEL_DIM), FF_DIM ** -0.5, 0.0),
    }


def pick_block(n_rows, heads, n_keys):
    q_block = n_rows
    while q_block % 2 == 0 and q_block * heads * n_keys > SCORE_CAP:
        q_block = q_block // 2
    return q_block


def rms_norm(values, gain_vec):
    values_f = values.astype(jnp.float32)
    inv_rms = lax.rsqrt(jnp.mean(values_f * values_f, axis=-1, keepdims=True) + NORM_EPS)
    return (values_f * inv_rms * gain_vec.astype(jnp.float32)).astype(jnp.bfloat16)


def rotate(values, cos_tab, sin_tab):
    half_dim = values.shape[-1] // 2
    first_half = values[..., :half_dim]
    second_half = values[..., half_dim:]
    return jnp.concatenate([first_half * cos_tab - second_half * sin_tab, second_half * cos_tab + first_half * sin_tab], axis=-1)


def attention(queries, keys_rot, values):
    seq_len, kv_heads, q_group, head_dim = queries.shape
    q_block = pick_block(seq_len, kv_heads * q_group, seq_len)
    n_blocks = seq_len // q_block
    score_scale = head_dim ** -0.5
    key_pos = jnp.arange(seq_len)
    key_f = keys_rot.astype(jnp.float32)
    value_f = values.astype(jnp.float32)

    def one_block(blk_args):
        q_blk, blk_idx = blk_args
        scores = jnp.einsum("qkgd,skd->kqgs", q_blk.astype(jnp.float32), key_f) * score_scale
        q_pos = blk_idx * q_block + jnp.arange(q_block)
        causal = (q_pos[:, None] >= key_pos[None, :])[None, :, None, :]
        scores = jnp.where(causal, scores, -jnp.inf)
        probs_bf = jax.nn.softmax(scores, axis=-1).astype(jnp.bfloat16)
        blk_out = jnp.einsum("kqgs,skd->qkgd", probs_bf.astype(jnp.float32), value_f)
        return blk_out.astype(jnp.bfloat16)

    q_blocks = queries.reshape(n_blocks, q_block, kv_heads, q_group, head_dim)
    blk_outs = lax.map(jax.checkpoint(one_block), (q_blocks, jnp.arange(n_blocks)))
    return blk_outs.reshape(seq_len, kv_heads * q_group * head_dim)


def decoder_layer(tokens, norm_attn, w_query, w_key, w_value, w_out, norm_mlp, w_gate, w_up, w_down):
    seq_len = tokens.shape[0]
    half_dim = HEAD_DIM // 2
    inv_freq = ROPE_BASE ** (-jnp.arange(half_dim, dtype=jnp.float32) * (2.0 / HEAD_DIM))
    angles = jnp.arange(seq_len, dtype=jnp.float32)[:, None] * inv_freq[None, :]
    cos_tab = jnp.cos(angles)[:, None, :]
    sin_tab = jnp.sin(angles)[:, None, :]
    normed = rms_norm(tokens, norm_attn)
    q_pre = jnp.dot(normed, w_query, preferred_element_type=jnp.float32).reshape(seq_len, Q_HEADS, HEAD_DIM)
    k_pre = jnp.dot(normed, w_key, preferred_element_type=jnp.float32).reshape(seq_len, KV_HEADS, HEAD_DIM)
    queries = rotate(q_pre, cos_tab, sin_tab).astype(jnp.bfloat16)
    keys_rot = rotate(k_pre, cos_tab, sin_tab).astype(jnp.bfloat16)
    values = jnp.dot(normed, w_value, preferred_element_type=jnp.float32).astype(jnp.bfloat16).reshape(seq_len, KV_HEADS, HEAD_DIM)
    attn_out = attention(queries.reshape(seq_len, KV_HEADS, Q_HEADS // KV_HEADS, HEAD_DIM), keys_rot, values)
    hidden = (tokens.astype(jnp.float32) + jnp.dot(attn_out, w_out, preferred_element_type=jnp.float32)).astype(jnp.bfloat16)
    normed_mlp = rms_norm(hidden, norm_mlp)
    gate_pre = jnp.dot(normed_mlp, w_gate, preferred_element_type=jnp.float32)
    up_pre = jnp.dot(normed_mlp, w_up, preferred_element_type=jnp.float32)
    mlp_act = (jax.nn.silu(gate_pre) * up_pre).astype(jnp.bfloat16)
    return (hidden.astype(jnp.float32) + jnp.dot(mlp_act, w_down, preferred_element_type=jnp.float32)).astype(jnp.bfloat16)


def reference(tokens, grad_out, norm_attn, w_query, w_key, w_value, w_out, norm_mlp, w_gate, w_up, w_down):
    weights = (norm_attn, w_query, w_key, w_value, w_out, norm_mlp, w_gate, w_up, w_down)

    def one_seq(grad_acc, seq_pair):
        seq_tok, seq_grad = seq_pair
        layer_out, pull_back = jax.vjp(decoder_layer, seq_tok, *weights)
        cotangents = pull_back(seq_grad)
        new_acc = tuple(acc_item + cot_item.astype(jnp.float32) for acc_item, cot_item in zip(grad_acc, cotangents[1:]))
        return new_acc, cotangents[0]

    zero_acc = tuple(jnp.zeros(weight.shape, jnp.float32) for weight in weights)
    grad_acc, grad_tokens = lax.scan(one_seq, zero_acc, (tokens, grad_out))
    inv_batch = 1.0 / tokens.shape[0]
    return (grad_tokens, grad_acc[0] * inv_batch, grad_acc[1] * inv_batch, grad_acc[2] * inv_batch, grad_acc[3] * inv_batch, grad_acc[4] * inv_batch, grad_acc[5] * inv_batch, grad_acc[6] * inv_batch, grad_acc[7] * inv_batch, grad_acc[8] * inv_batch)
```

```python
import functools
import math

import jax
import jax.numpy as jnp
from jax import lax
from jax.experimental import pallas as pl
from jax.experimental.pallas import tpu as pltpu
from jax.sharding import PartitionSpec as P


NORM_EPS = 1.0e-5
ROPE_BASE = 1.0e6
HEAD_DIM = 128
F32 = jnp.float32
BF16 = jnp.bfloat16
VMEM_LIMIT = 60 * 1024 * 1024
NEG = -1.0e30


def nn(a, b):
    return lax.dot_general(a, b, (((1,), (0,)), ((), ())), preferred_element_type=F32)


def nt(a, b):
    return lax.dot_general(a, b, (((1,), (1,)), ((), ())), preferred_element_type=F32)


def tn(a, b):
    return lax.dot_general(a, b, (((0,), (0,)), ((), ())), preferred_element_type=F32)


def norm_fwd(values, gain_vec):
    values_f = values.astype(F32)
    inv_rms = lax.rsqrt(jnp.mean(values_f * values_f, axis=-1, keepdims=True) + NORM_EPS)
    unit_vals = values_f * inv_rms
    return (unit_vals * gain_vec.astype(F32)).astype(BF16), unit_vals, inv_rms


def norm_bwd(grad_normed, unit_vals, inv_rms, gain_vec):
    grad_f = grad_normed.astype(F32)
    grad_gain = jnp.sum(grad_f * unit_vals, axis=0)
    grad_unit = grad_f * gain_vec.astype(F32)
    grad_in = inv_rms * (grad_unit - unit_vals * jnp.mean(grad_unit * unit_vals, axis=-1, keepdims=True))
    return grad_in, grad_gain


def rope_tables(positions):
    half_dim = HEAD_DIM // 2
    inv_freq = ROPE_BASE ** (-jnp.arange(half_dim, dtype=F32) * (2.0 / HEAD_DIM))
    angles = positions.astype(F32)[:, None] * inv_freq[None, :]
    cos, sin = jnp.cos(angles), jnp.sin(angles)
    return jnp.concatenate([cos, cos], axis=-1), jnp.concatenate([-sin, sin], axis=-1)


def rope(values, cos_tab, sin_tab):
    return values * cos_tab + pltpu.roll(values, HEAD_DIM // 2, 1) * sin_tab


def call(kernel, flops, moved, **kwargs):
    params = pltpu.CompilerParams(vmem_limit_bytes=VMEM_LIMIT)
    cost = pl.CostEstimate(flops=int(flops), bytes_accessed=int(moved), transcendentals=0)
    return pl.pallas_call(kernel, compiler_params=params, cost_estimate=cost, **kwargs)


def whole(shape):
    return pl.BlockSpec(shape, lambda *_: (0,) * len(shape))


def qkv_kernel(x_ref, wq_ref, wk_ref, wv_ref, cos_ref, sin_ref, out_ref):
    x, cos, sin = x_ref[...], cos_ref[...], sin_ref[...]
    q = nn(x, wq_ref[...])
    width = q.shape[1]
    for start in range(0, width, HEAD_DIM):
        out_ref[0, :, start : start + HEAD_DIM] = rope(q[:, start : start + HEAD_DIM], cos, sin).astype(BF16)
    out_ref[0, :, width : width + HEAD_DIM] = rope(nn(x, wk_ref[...]), cos, sin).astype(BF16)
    out_ref[0, :, width + HEAD_DIM : width + 2 * HEAD_DIM] = nn(x, wv_ref[...]).astype(BF16)


def qkv_heads(normed, w_query, w_key, w_value, cos, sin, groups):
    tok, dim = normed.shape
    qw = w_query.shape[1] // groups
    kw = w_key.shape[1] // groups
    return call(
        qkv_kernel,
        2 * tok * dim * (qw + 2 * kw) * groups,
        2 * dim * (qw + 2 * kw) * groups,
        grid=(groups,),
        in_specs=[
            whole((tok, dim)),
            pl.BlockSpec((dim, qw), lambda j: (0, j)),
            pl.BlockSpec((dim, kw), lambda j: (0, j)),
            pl.BlockSpec((dim, kw), lambda j: (0, j)),
            whole((tok, HEAD_DIM)),
            whole((tok, HEAD_DIM)),
        ],
        out_specs=pl.BlockSpec((1, tok, qw + 2 * kw), lambda j: (j, 0, 0)),
        out_shape=jax.ShapeDtypeStruct((groups, tok, qw + 2 * kw), BF16),
        name="qkv",
    )(normed, w_query, w_key, w_value, cos, sin)


def attn_fwd_kernel(blk, n_q, qkv_ref, out_ref, lse_ref, *scrs):
    i = pl.program_id(0)
    coef = HEAD_DIM**-0.5 * math.log2(math.e)
    k_at, v_at = n_q * HEAD_DIM, (n_q + 1) * HEAD_DIM
    rows = pl.ds(pl.multiple_of(i * blk, blk), blk)
    lanes = lambda t, op: functools.reduce(op, [t[:, s : s + 128] for s in range(0, blk, 128)])
    qs = [qkv_ref[rows, h * HEAD_DIM : (h + 1) * HEAD_DIM] for h in range(n_q)]
    causal = lax.broadcasted_iota(jnp.int32, (blk, blk), 0) >= lax.broadcasted_iota(jnp.int32, (blk, blk), 1)
    at = lambda j: pl.ds(pl.multiple_of(j * blk, blk), blk)

    def score_step(j, tops, masked):
        key = qkv_ref[at(j), k_at:v_at]
        new = []
        for h in range(n_q):
            s = nt(qs[h], key)
            if masked:
                s = jnp.where(causal, s, NEG)
            scrs[h][:, at(j)] = s
            new.append(jnp.maximum(tops[h], lanes(s, jnp.maximum)))
        return tuple(new)

    start = tuple(jnp.full((blk, 128), NEG, F32) for _ in range(n_q))
    tops = lax.fori_loop(0, i, lambda j, t: score_step(j, t, False), start)
    tops = score_step(i, tops, True)
    row_max = [jnp.max(t, axis=1, keepdims=True) for t in tops]

    def exp_step(j, sums):
        new = []
        for h in range(n_q):
            e = jnp.exp2((scrs[h][:, at(j)] - row_max[h]) * coef)
            scrs[h][:, at(j)] = e
            new.append(sums[h] + lanes(e, jnp.add))
        return tuple(new)

    sums = lax.fori_loop(0, i + 1, exp_step, tuple(jnp.zeros((blk, 128), F32) for _ in range(n_q)))
    row_sum = [jnp.sum(t, axis=1, keepdims=True) for t in sums]
    inv_sum = [1.0 / t for t in row_sum]

    def out_step(j, accs):
        value = qkv_ref[at(j), v_at : v_at + HEAD_DIM]
        return tuple(accs[h] + nn((scrs[h][:, at(j)] * inv_sum[h]).astype(BF16), value) for h in range(n_q))

    accs = lax.fori_loop(0, i + 1, out_step, tuple(jnp.zeros((blk, HEAD_DIM), F32) for _ in range(n_q)))
    for h in range(n_q):
        out_ref[:, h * HEAD_DIM : (h + 1) * HEAD_DIM] = accs[h].astype(BF16)
        log_norm = row_max[h] * coef + jnp.log2(row_sum[h])
        lse_ref[h * 8 : (h + 1) * 8, :] = jnp.transpose(jnp.broadcast_to(log_norm, (blk, 128)))[:8, :]


def attn_fwd(qkv, blk):
    seq, width = qkv.shape
    n_q = width // HEAD_DIM - 2
    return call(
        functools.partial(attn_fwd_kernel, blk, n_q),
        2 * n_q * seq * seq * HEAD_DIM * 2,
        seq * width * 2,
        grid=(seq // blk,),
        in_specs=[whole((seq, width))],
        out_specs=[pl.BlockSpec((blk, n_q * HEAD_DIM), lambda i: (i, 0)), pl.BlockSpec((8 * n_q, blk), lambda i: (0, i))],
        out_shape=[jax.ShapeDtypeStruct((seq, n_q * HEAD_DIM), BF16), jax.ShapeDtypeStruct((8 * n_q, seq), F32)],
        scratch_shapes=[pltpu.VMEM((blk, seq), F32)] * n_q,
        name="attn_fwd",
    )(qkv)


def attn_bwd_kernel(blk, n_q, qkv_ref, do_ref, lse_ref, cos_ref, sin_ref, out_ref, dk_scr, dv_scr, *scrs):
    i, steps = pl.program_id(0), pl.num_programs(0)
    scale = HEAD_DIM**-0.5
    coef = scale * math.log2(math.e)
    k_at, v_at = n_q * HEAD_DIM, (n_q + 1) * HEAD_DIM
    at = lambda j: pl.ds(pl.multiple_of(j * blk, blk), blk)
    p_scrs, dp_scrs = scrs[:n_q], scrs[n_q:]
    qs = [qkv_ref[at(i), h * HEAD_DIM : (h + 1) * HEAD_DIM] for h in range(n_q)]
    dos = [do_ref[:, h * HEAD_DIM : (h + 1) * HEAD_DIM] for h in range(n_q)]
    lses = [lse_ref[h * 8 : h * 8 + 1, :] for h in range(n_q)]
    causal = lax.broadcasted_iota(jnp.int32, (blk, blk), 0) <= lax.broadcasted_iota(jnp.int32, (blk, blk), 1)

    @pl.when(i == 0)
    def _():
        dk_scr[...] = jnp.zeros_like(dk_scr)
        dv_scr[...] = jnp.zeros_like(dv_scr)

    def prob_step(j, dots, masked):
        key, value = qkv_ref[at(j), k_at:v_at], qkv_ref[at(j), v_at : v_at + HEAD_DIM]
        new, dv = [], dv_scr[at(j), :]
        for h in range(n_q):
            p = jnp.exp2(nt(key, qs[h]) * coef - lses[h])
            if masked:
                p = jnp.where(causal, p, 0.0)
            dp = nt(value, dos[h]).astype(BF16)
            p_scrs[h][at(j), :] = p
            dp_scrs[h][at(j), :] = dp
            dv = dv + nn(p.astype(BF16), dos[h])
            new.append(dots[h] + jnp.sum((p * dp.astype(F32)).reshape(blk // 8, 8, blk), axis=0))
        dv_scr[at(j), :] = dv
        return tuple(new)

    dots = lax.fori_loop(0, i, lambda j, t: prob_step(j, t, False), tuple(jnp.zeros((8, blk), F32) for _ in range(n_q)))
    dots = prob_step(i, dots, True)
    row_dot = [jnp.sum(t, axis=0, keepdims=True) for t in dots]

    def grad_step(j, accs):
        key = qkv_ref[at(j), k_at:v_at]
        new, dk = [], dk_scr[at(j), :]
        for h in range(n_q):
            ds = (p_scrs[h][at(j), :] * (dp_scrs[h][at(j), :].astype(F32) - row_dot[h]) * scale).astype(BF16)
            dk = dk + nn(ds, qs[h])
            new.append(accs[h] + tn(ds, key))
        dk_scr[at(j), :] = dk
        return tuple(new)

    accs = lax.fori_loop(0, i + 1, grad_step, tuple(jnp.zeros((blk, HEAD_DIM), F32) for _ in range(n_q)))
    unrope = lambda g, sl: rope(g.astype(BF16).astype(F32), cos_ref[sl, :], -sin_ref[sl, :]).astype(BF16)
    for h in range(n_q):
        out_ref[at(i), h * HEAD_DIM : (h + 1) * HEAD_DIM] = unrope(accs[h], at(i))

    @pl.when(i == steps - 1)
    def _():
        def finish(j, carry):
            out_ref[at(j), k_at:v_at] = unrope(dk_scr[at(j), :], at(j))
            out_ref[at(j), v_at : v_at + HEAD_DIM] = dv_scr[at(j), :].astype(BF16)
            return carry

        lax.fori_loop(0, steps, finish, 0)


def attn_bwd(qkv, grad_out, lse, cos, sin, blk):
    seq, width = qkv.shape
    n_q = width // HEAD_DIM - 2
    return call(
        functools.partial(attn_bwd_kernel, blk, n_q),
        5 * n_q * seq * seq * HEAD_DIM * 2,
        seq * width * 4,
        grid=(seq // blk,),
        in_specs=[
            whole((seq, width)),
            pl.BlockSpec((blk, n_q * HEAD_DIM), lambda i: (i, 0)),
            pl.BlockSpec((8 * n_q, blk), lambda i: (0, i)),
            whole((seq, HEAD_DIM)),
            whole((seq, HEAD_DIM)),
        ],
        out_specs=whole((seq, width)),
        out_shape=jax.ShapeDtypeStruct((seq, width), BF16),
        scratch_shapes=[pltpu.VMEM((seq, HEAD_DIM), F32)] * 2
        + [pltpu.VMEM((seq, blk), F32)] * n_q
        + [pltpu.VMEM((seq, blk), BF16)] * n_q,
        name="attn_bwd",
    )(qkv, grad_out, lse, cos, sin)


def act_grads(gate, up, grad_act):
    sig = 1.0 / (1.0 + jnp.exp(-gate))
    act = gate * sig
    grad_gate = (grad_act * up * sig * (1.0 + gate * (1.0 - sig))).astype(BF16)
    grad_up = (grad_act * act).astype(BF16)
    return (act * up).astype(BF16), grad_gate, grad_up


def mlp_kernel(m_ref, dy_ref, wg_ref, wu_ref, wd_ref, out_ref, acc_ref):
    step = pl.program_id(0)
    m, dy = m_ref[...], dy_ref[...]
    grad_act = nt(dy, wd_ref[...]).astype(BF16).astype(F32)
    _, grad_gate, grad_up = act_grads(nn(m, wg_ref[...]), nn(m, wu_ref[...]), grad_act)
    total = nt(grad_gate, wg_ref[...]) + nt(grad_up, wu_ref[...])

    @pl.when(step == 0)
    def _():
        acc_ref[...] = total

    @pl.when(step > 0)
    def _():
        acc_ref[...] += total

    @pl.when(step == pl.num_programs(0) - 1)
    def _():
        out_ref[...] = acc_ref[...].astype(BF16)


def mlp_grad_input(m, dy, w_gate, w_up, w_down, blk):
    tok, dim = m.shape
    width = w_gate.shape[1]
    return call(
        mlp_kernel,
        5 * 2 * tok * dim * width,
        3 * 2 * dim * width,
        grid=(width // blk,),
        in_specs=[
            whole((tok, dim)),
            whole((tok, dim)),
            pl.BlockSpec((dim, blk), lambda j: (0, j)),
            pl.BlockSpec((dim, blk), lambda j: (0, j)),
            pl.BlockSpec((blk, dim), lambda j: (j, 0)),
        ],
        out_specs=whole((tok, dim)),
        out_shape=jax.ShapeDtypeStruct((tok, dim), BF16),
        scratch_shapes=[pltpu.VMEM((tok, dim), F32)],
        name="mlp_grad_input",
    )(m, dy, w_gate, w_up, w_down)


def spread_kernel(groups, widths, in_ref, *out_refs):
    rows = in_ref.shape[0] // groups
    for g in range(groups):
        at = 0
        for width, out_ref in zip(widths, out_refs):
            piece = in_ref[g * rows : (g + 1) * rows, at : at + width]
            out_ref[:, g * width : (g + 1) * width] = piece.astype(F32)
            at += width


def spread(stacked, outer, groups, widths):
    total, row_width = stacked.shape
    rows = total // (outer * groups)
    return call(
        functools.partial(spread_kernel, groups, widths),
        total * row_width,
        total * row_width * 6,
        grid=(outer,),
        in_specs=[pl.BlockSpec((groups * rows, row_width), lambda o: (o, 0))],
        out_specs=[pl.BlockSpec((rows, groups * width), lambda o: (o, 0)) for width in widths],
        out_shape=[jax.ShapeDtypeStruct((outer * rows, groups * width), F32) for width in widths],
        name="spread",
    )(stacked)


def solution(mesh):
    sp_size = mesh.shape["sp"]
    dp_size = mesh.shape["dp"]
    seq_spec = P("dp", "sp", None)
    inv_batch = 1.0 / dp_size

    def device_step(tokens, grad_out, norm_attn, w_query, w_key, w_value, w_out, norm_mlp, w_gate, w_up, w_down):
        x = tokens[0]
        dy = grad_out[0]
        sp_idx = lax.axis_index("sp")
        n_local, dim = x.shape
        n_seq = n_local * sp_size
        q_width = w_query.shape[1] // sp_size
        k_width = w_key.shape[1] // sp_size
        ff_local = w_gate.shape[1] // sp_size
        attn_blk = min(512, n_seq // 2)
        cos_all, sin_all = rope_tables(jnp.arange(n_seq))
        cos_loc, sin_loc = rope_tables(sp_idx * n_local + jnp.arange(n_local))

        def to_heads(stacked):
            return lax.all_to_all(stacked, "sp", 0, 0, tiled=True)

        def gather_seq(local):
            return lax.all_gather(local, "sp", axis=0, tiled=True)

        def reduce_dp(grad):
            pieces = grad.astype(BF16).reshape(dp_size, grad.shape[0] // dp_size, grad.shape[1])
            pieces = lax.all_to_all(pieces, "dp", 0, 0, tiled=True)
            return (jnp.sum(pieces.astype(F32), axis=0) * inv_batch).astype(BF16)

        dy_full = gather_seq(dy)
        normed, unit_attn, inv_attn = norm_fwd(x, norm_attn)
        qkv_loc = qkv_heads(normed, w_query, w_key, w_value, cos_loc, sin_loc, sp_size)
        qkv = to_heads(qkv_loc).reshape(n_seq, q_width + 2 * k_width)
        attn, lse = attn_fwd(qkv, attn_blk)
        attn_tok = to_heads(attn.reshape(sp_size, n_local, q_width))
        w_out_heads = w_out.reshape(sp_size, q_width, dim)
        projected = jnp.einsum("jte,jed->td", attn_tok, w_out_heads, preferred_element_type=F32)
        hidden = (x.astype(F32) + projected).astype(BF16)
        normed_mlp, unit_mlp, inv_mlp = norm_fwd(hidden, norm_mlp)
        m_full = gather_seq(normed_mlp)

        grad_m = mlp_grad_input(normed_mlp, dy, w_gate, w_up, w_down, min(512, w_gate.shape[1]))
        grad_hid_norm, g_norm_mlp = norm_bwd(grad_m, unit_mlp, inv_mlp, norm_mlp)
        grad_hidden = (dy.astype(F32) + grad_hid_norm).astype(BF16)
        grad_attn = jnp.einsum("td,jed->jte", grad_hidden, w_out_heads, preferred_element_type=F32).astype(BF16)
        grad_attn = to_heads(grad_attn).reshape(n_seq, q_width)
        normed_full = gather_seq(normed)
        grad_hidden_full = gather_seq(grad_hidden)

        my_gate = lax.dynamic_slice_in_dim(w_gate, sp_idx * ff_local, ff_local, 1)
        my_up = lax.dynamic_slice_in_dim(w_up, sp_idx * ff_local, ff_local, 1)
        my_down = lax.dynamic_slice_in_dim(w_down, sp_idx * ff_local, ff_local, 0)
        gate = nn(m_full, my_gate)
        up = nn(m_full, my_up)
        grad_act = nt(dy_full, my_down).astype(BF16)
        mlp_act, grad_gate, grad_up = act_grads(gate, up, grad_act.astype(F32))

        red_down = reduce_dp(tn(mlp_act, dy_full))
        red_gate = reduce_dp(tn(m_full, grad_gate))
        red_up = reduce_dp(tn(m_full, grad_up))
        g_down = lax.all_gather(red_down, ("sp", "dp"), axis=0, tiled=True)
        g_gate = lax.all_gather(red_gate, ("dp", "sp"), axis=0, tiled=True)
        g_up = lax.all_gather(red_up, ("dp", "sp"), axis=0, tiled=True)

        gqkv = attn_bwd(qkv, grad_attn, lse, cos_all, sin_all, attn_blk)
        red_out = reduce_dp(tn(attn, grad_hidden_full))
        red_qkv = reduce_dp(tn(normed_full, gqkv))
        g_out = lax.all_gather(red_out, ("sp", "dp"), axis=0, tiled=True)
        g_qkv = lax.all_gather(red_qkv, ("dp", "sp"), axis=0, tiled=True)

        gqkv_tok = to_heads(gqkv.reshape(sp_size, n_local, q_width + 2 * k_width))
        flat = lambda t: jnp.transpose(t, (1, 0, 2)).reshape(n_local, -1)
        grad_normed = (
            nt(flat(gqkv_tok[:, :, :q_width]), w_query)
            + nt(flat(gqkv_tok[:, :, q_width : q_width + k_width]), w_key)
            + nt(flat(gqkv_tok[:, :, q_width + k_width :]), w_value)
        ).astype(BF16)
        grad_tok_norm, g_norm_attn = norm_bwd(grad_normed, unit_attn, inv_attn, norm_attn)
        grad_tokens = (grad_hidden.astype(F32) + grad_tok_norm).astype(BF16)

        gains = lax.all_gather(jnp.concatenate([g_norm_attn, g_norm_mlp])[None], ("dp", "sp"), axis=0, tiled=True)
        gains = jnp.sum(gains, axis=0) * inv_batch

        (g_gate,) = spread(g_gate, dp_size, sp_size, (ff_local,))
        (g_up,) = spread(g_up, dp_size, sp_size, (ff_local,))
        g_query, g_key, g_value = spread(g_qkv, dp_size, sp_size, (q_width, k_width, k_width))
        return (
            grad_tokens[None],
            gains[:dim],
            g_query,
            g_key,
            g_value,
            g_out.astype(F32),
            gains[dim:],
            g_gate,
            g_up,
            g_down.astype(F32),
        )

    return jax.shard_map(device_step, mesh=mesh, in_specs=(seq_spec, seq_spec) + (P(),) * 9, out_specs=(seq_spec,) + (P(),) * 9, check_vma=False)
```

```python
import functools
import math

import jax
import jax.numpy as jnp
from jax import lax
from jax.experimental import pallas as pl
from jax.experimental.pallas import tpu as pltpu
from jax.sharding import PartitionSpec as P


NORM_EPS = 1.0e-5
ROPE_BASE = 1.0e6
HEAD_DIM = 128
F32 = jnp.float32
BF16 = jnp.bfloat16
VMEM_LIMIT = 60 * 1024 * 1024
MESH = pl.DeviceIdType.MESH
NEG = -1.0e30


def nn(a, b):
    return lax.dot_general(a, b, (((1,), (0,)), ((), ())), preferred_element_type=F32)


def nt(a, b):
    return lax.dot_general(a, b, (((1,), (1,)), ((), ())), preferred_element_type=F32)


def tn(a, b):
    return lax.dot_general(a, b, (((0,), (0,)), ((), ())), preferred_element_type=F32)


def norm_fwd(values, gain_vec):
    values_f = values.astype(F32)
    inv_rms = lax.rsqrt(jnp.mean(values_f * values_f, axis=-1, keepdims=True) + NORM_EPS)
    unit_vals = values_f * inv_rms
    return (unit_vals * gain_vec.astype(F32)).astype(BF16), unit_vals, inv_rms


def norm_bwd(grad_normed, unit_vals, inv_rms, gain_vec):
    grad_f = grad_normed.astype(F32)
    grad_gain = jnp.sum(grad_f * unit_vals, axis=0)
    grad_unit = grad_f * gain_vec.astype(F32)
    grad_in = inv_rms * (grad_unit - unit_vals * jnp.mean(grad_unit * unit_vals, axis=-1, keepdims=True))
    return grad_in, grad_gain


def rope_tables(positions):
    half_dim = HEAD_DIM // 2
    inv_freq = ROPE_BASE ** (-jnp.arange(half_dim, dtype=F32) * (2.0 / HEAD_DIM))
    angles = positions.astype(F32)[:, None] * inv_freq[None, :]
    cos, sin = jnp.cos(angles), jnp.sin(angles)
    return jnp.concatenate([cos, cos], axis=-1), jnp.concatenate([-sin, sin], axis=-1)


def rope(values, cos_tab, sin_tab):
    return values * cos_tab + pltpu.roll(values, HEAD_DIM // 2, 1) * sin_tab


def call(kernel, flops, moved, **kwargs):
    params = pltpu.CompilerParams(vmem_limit_bytes=VMEM_LIMIT)
    cost = pl.CostEstimate(flops=int(flops), bytes_accessed=int(moved), transcendentals=0)
    return pl.pallas_call(kernel, compiler_params=params, cost_estimate=cost, **kwargs)


def whole(shape):
    return pl.BlockSpec(shape, lambda *_: (0,) * len(shape))


def qkv_kernel(idx_ref, x_ref, wq_ref, wk_ref, wv_ref, cos_ref, sin_ref, out_ref):
    x, cos, sin = x_ref[...], cos_ref[...], sin_ref[...]
    q = nn(x, wq_ref[...])
    width = q.shape[1]
    for start in range(0, width, HEAD_DIM):
        out_ref[:, start : start + HEAD_DIM] = rope(q[:, start : start + HEAD_DIM], cos, sin).astype(BF16)
    kv = nn(x, jnp.concatenate([wk_ref[...], wv_ref[...]], axis=1))
    out_ref[:, width : width + HEAD_DIM] = rope(kv[:, :HEAD_DIM], cos, sin).astype(BF16)
    out_ref[:, width + HEAD_DIM : width + 2 * HEAD_DIM] = kv[:, HEAD_DIM:].astype(BF16)


def qkv_heads(normed, w_query, w_key, w_value, cos, sin, groups, idx):
    seq, dim = normed.shape
    qw = w_query.shape[1] // groups
    kw = w_key.shape[1] // groups
    blk = min(512, seq)
    return pl.pallas_call(
        qkv_kernel,
        grid_spec=pltpu.PrefetchScalarGridSpec(
            num_scalar_prefetch=1,
            grid=(seq // blk,),
            in_specs=[
                pl.BlockSpec((blk, dim), lambda i, idx: (i, 0)),
                pl.BlockSpec((dim, qw), lambda i, idx: (0, idx[0])),
                pl.BlockSpec((dim, kw), lambda i, idx: (0, idx[0])),
                pl.BlockSpec((dim, kw), lambda i, idx: (0, idx[0])),
                pl.BlockSpec((blk, HEAD_DIM), lambda i, idx: (i, 0)),
                pl.BlockSpec((blk, HEAD_DIM), lambda i, idx: (i, 0)),
            ],
            out_specs=pl.BlockSpec((blk, qw + 2 * kw), lambda i, idx: (i, 0)),
        ),
        out_shape=jax.ShapeDtypeStruct((seq, qw + 2 * kw), BF16),
        compiler_params=pltpu.CompilerParams(vmem_limit_bytes=VMEM_LIMIT),
        cost_estimate=pl.CostEstimate(flops=2 * seq * dim * (qw + 2 * kw), bytes_accessed=4 * seq * dim, transcendentals=0),
        name="qkv",
    )(idx.reshape(1).astype(jnp.int32), normed, w_query, w_key, w_value, cos, sin)


def attn_fwd_kernel(blk, n_q, qkv_ref, out_ref, lse_ref, *scrs):
    i = pl.program_id(0)
    coef = HEAD_DIM**-0.5 * math.log2(math.e)
    k_at, v_at = n_q * HEAD_DIM, (n_q + 1) * HEAD_DIM
    rows = pl.ds(pl.multiple_of(i * blk, blk), blk)
    lanes = lambda t, op: functools.reduce(op, [t[:, s : s + 128] for s in range(0, blk, 128)])
    qs = [qkv_ref[rows, h * HEAD_DIM : (h + 1) * HEAD_DIM] for h in range(n_q)]
    causal = lax.broadcasted_iota(jnp.int32, (blk, blk), 0) >= lax.broadcasted_iota(jnp.int32, (blk, blk), 1)
    at = lambda j: pl.ds(pl.multiple_of(j * blk, blk), blk)

    def score_step(j, tops, masked):
        key = qkv_ref[at(j), k_at:v_at]
        new = []
        for h in range(n_q):
            s = nt(qs[h], key)
            if masked:
                s = jnp.where(causal, s, NEG)
            scrs[h][:, at(j)] = s
            new.append(jnp.maximum(tops[h], lanes(s, jnp.maximum)))
        return tuple(new)

    start = tuple(jnp.full((blk, 128), NEG, F32) for _ in range(n_q))
    tops = lax.fori_loop(0, i, lambda j, t: score_step(j, t, False), start)
    tops = score_step(i, tops, True)
    row_max = [jnp.max(t, axis=1, keepdims=True) for t in tops]

    def exp_step(j, sums):
        new = []
        for h in range(n_q):
            e = jnp.exp2((scrs[h][:, at(j)] - row_max[h]) * coef)
            scrs[h][:, at(j)] = e
            new.append(sums[h] + lanes(e, jnp.add))
        return tuple(new)

    sums = lax.fori_loop(0, i + 1, exp_step, tuple(jnp.zeros((blk, 128), F32) for _ in range(n_q)))
    row_sum = [jnp.sum(t, axis=1, keepdims=True) for t in sums]
    inv_sum = [1.0 / t for t in row_sum]

    def out_step(j, accs):
        value = qkv_ref[at(j), v_at : v_at + HEAD_DIM]
        return tuple(accs[h] + nn((scrs[h][:, at(j)] * inv_sum[h]).astype(BF16), value) for h in range(n_q))

    accs = lax.fori_loop(0, i + 1, out_step, tuple(jnp.zeros((blk, HEAD_DIM), F32) for _ in range(n_q)))
    for h in range(n_q):
        out_ref[:, h * HEAD_DIM : (h + 1) * HEAD_DIM] = accs[h].astype(BF16)
        log_norm = row_max[h] * coef + jnp.log2(row_sum[h])
        lse_ref[h * 8 : (h + 1) * 8, :] = jnp.transpose(jnp.broadcast_to(log_norm, (blk, 128)))[:8, :]


def attn_fwd(qkv, blk):
    seq, width = qkv.shape
    n_q = width // HEAD_DIM - 2
    return call(
        functools.partial(attn_fwd_kernel, blk, n_q),
        2 * n_q * seq * seq * HEAD_DIM * 2,
        seq * width * 2,
        grid=(seq // blk,),
        in_specs=[whole((seq, width))],
        out_specs=[pl.BlockSpec((blk, n_q * HEAD_DIM), lambda i: (i, 0)), pl.BlockSpec((8 * n_q, blk), lambda i: (0, i))],
        out_shape=[jax.ShapeDtypeStruct((seq, n_q * HEAD_DIM), BF16), jax.ShapeDtypeStruct((8 * n_q, seq), F32)],
        scratch_shapes=[pltpu.VMEM((blk, seq), F32)] * n_q,
        name="attn_fwd",
    )(qkv)


def attn_bwd_kernel(blk, n_q, qkv_ref, do_ref, lse_ref, cos_ref, sin_ref, out_ref, dk_scr, dv_scr, *scrs):
    i, steps = pl.program_id(0), pl.num_programs(0)
    scale = HEAD_DIM**-0.5
    coef = scale * math.log2(math.e)
    k_at, v_at = n_q * HEAD_DIM, (n_q + 1) * HEAD_DIM
    at = lambda j: pl.ds(pl.multiple_of(j * blk, blk), blk)
    p_scrs, dp_scrs = scrs[:n_q], scrs[n_q:]
    qs = [qkv_ref[at(i), h * HEAD_DIM : (h + 1) * HEAD_DIM] for h in range(n_q)]
    dos = [do_ref[:, h * HEAD_DIM : (h + 1) * HEAD_DIM] for h in range(n_q)]
    lses = [lse_ref[h * 8 : h * 8 + 1, :] for h in range(n_q)]
    causal = lax.broadcasted_iota(jnp.int32, (blk, blk), 0) <= lax.broadcasted_iota(jnp.int32, (blk, blk), 1)

    @pl.when(i == 0)
    def _():
        dk_scr[...] = jnp.zeros_like(dk_scr)
        dv_scr[...] = jnp.zeros_like(dv_scr)

    def prob_step(j, dots, masked):
        key, value = qkv_ref[at(j), k_at:v_at], qkv_ref[at(j), v_at : v_at + HEAD_DIM]
        new, dv = [], dv_scr[at(j), :]
        for h in range(n_q):
            p = jnp.exp2(nt(key, qs[h]) * coef - lses[h])
            if masked:
                p = jnp.where(causal, p, 0.0)
            dp = nt(value, dos[h]).astype(BF16)
            p_scrs[h][at(j), :] = p
            dp_scrs[h][at(j), :] = dp
            dv = dv + nn(p.astype(BF16), dos[h])
            new.append(dots[h] + jnp.sum((p * dp.astype(F32)).reshape(blk // 8, 8, blk), axis=0))
        dv_scr[at(j), :] = dv
        return tuple(new)

    dots = lax.fori_loop(0, i, lambda j, t: prob_step(j, t, False), tuple(jnp.zeros((8, blk), F32) for _ in range(n_q)))
    dots = prob_step(i, dots, True)
    row_dot = [jnp.sum(t, axis=0, keepdims=True) for t in dots]

    def grad_step(j, accs):
        key = qkv_ref[at(j), k_at:v_at]
        new, dk = [], dk_scr[at(j), :]
        for h in range(n_q):
            ds = (p_scrs[h][at(j), :] * (dp_scrs[h][at(j), :].astype(F32) - row_dot[h]) * scale).astype(BF16)
            dk = dk + nn(ds, qs[h])
            new.append(accs[h] + tn(ds, key))
        dk_scr[at(j), :] = dk
        return tuple(new)

    accs = lax.fori_loop(0, i + 1, grad_step, tuple(jnp.zeros((blk, HEAD_DIM), F32) for _ in range(n_q)))
    unrope = lambda g, sl: rope(g.astype(BF16).astype(F32), cos_ref[sl, :], -sin_ref[sl, :]).astype(BF16)
    for h in range(n_q):
        out_ref[at(i), h * HEAD_DIM : (h + 1) * HEAD_DIM] = unrope(accs[h], at(i))

    @pl.when(i == steps - 1)
    def _():
        def finish(j, carry):
            out_ref[at(j), k_at:v_at] = unrope(dk_scr[at(j), :], at(j))
            out_ref[at(j), v_at : v_at + HEAD_DIM] = dv_scr[at(j), :].astype(BF16)
            return carry

        lax.fori_loop(0, steps, finish, 0)


def attn_bwd(qkv, grad_out, lse, cos, sin, blk):
    seq, width = qkv.shape
    n_q = width // HEAD_DIM - 2
    return call(
        functools.partial(attn_bwd_kernel, blk, n_q),
        5 * n_q * seq * seq * HEAD_DIM * 2,
        seq * width * 4,
        grid=(seq // blk,),
        in_specs=[
            whole((seq, width)),
            pl.BlockSpec((blk, n_q * HEAD_DIM), lambda i: (i, 0)),
            pl.BlockSpec((8 * n_q, blk), lambda i: (0, i)),
            whole((seq, HEAD_DIM)),
            whole((seq, HEAD_DIM)),
        ],
        out_specs=whole((seq, width)),
        out_shape=jax.ShapeDtypeStruct((seq, width), BF16),
        scratch_shapes=[pltpu.VMEM((seq, HEAD_DIM), F32)] * 2
        + [pltpu.VMEM((seq, blk), F32)] * n_q
        + [pltpu.VMEM((seq, blk), BF16)] * n_q,
        name="attn_bwd",
    )(qkv, grad_out, lse, cos, sin)


def act_grads(gate, up, grad_act):
    sig = 1.0 / (1.0 + jnp.exp(-gate))
    act = gate * sig
    grad_gate = (grad_act * up * sig * (1.0 + gate * (1.0 - sig))).astype(BF16)
    grad_up = (grad_act * act).astype(BF16)
    return (act * up).astype(BF16), grad_gate, grad_up


def mlp_kernel(m_ref, dy_ref, wg_ref, wu_ref, wd_ref, out_ref, acc_ref):
    step = pl.program_id(0)
    m, dy = m_ref[...], dy_ref[...]
    grad_act = nt(dy, wd_ref[...]).astype(BF16).astype(F32)
    _, grad_gate, grad_up = act_grads(nn(m, wg_ref[...]), nn(m, wu_ref[...]), grad_act)
    total = nt(grad_gate, wg_ref[...]) + nt(grad_up, wu_ref[...])

    @pl.when(step == 0)
    def _():
        acc_ref[...] = total

    @pl.when(step > 0)
    def _():
        acc_ref[...] += total

    @pl.when(step == pl.num_programs(0) - 1)
    def _():
        out_ref[...] = acc_ref[...].astype(BF16)


def mlp_grad_input(m, dy, w_gate, w_up, w_down, blk):
    tok, dim = m.shape
    width = w_gate.shape[1]
    return call(
        mlp_kernel,
        5 * 2 * tok * dim * width,
        3 * 2 * dim * width,
        grid=(width // blk,),
        in_specs=[
            whole((tok, dim)),
            whole((tok, dim)),
            pl.BlockSpec((dim, blk), lambda j: (0, j)),
            pl.BlockSpec((dim, blk), lambda j: (0, j)),
            pl.BlockSpec((blk, dim), lambda j: (j, 0)),
        ],
        out_specs=whole((tok, dim)),
        out_shape=jax.ShapeDtypeStruct((tok, dim), BF16),
        scratch_shapes=[pltpu.VMEM((tok, dim), F32)],
        name="mlp_grad_input",
    )(m, dy, w_gate, w_up, w_down)


class Ring:
    def __init__(self, n, subs, slow, fast, source, recv1, acc, send2, recv2, s1, r1, s2, r2):
        self.n, self.subs, self.slow, self.fast, self.source = n, subs, slow, fast, source
        self.recv1, self.acc, self.send2, self.recv2 = recv1, acc, send2, recv2
        self.s1, self.r1, self.s2, self.r2 = s1, r1, s2, r2
        self.z, self.y = lax.axis_index(slow), lax.axis_index(fast)
        self.height = recv1.shape[5]

    def wrap(self, v):
        return lax.rem(v + 2 * self.n, self.n)

    def goal(self, c, phase):
        step = 1 - 2 * (c % 2)
        if (c < 2) == (phase == 1):
            return {self.fast: self.wrap(self.y + step)}
        return {self.slow: self.wrap(self.z + step)}

    def arrive(self):
        barrier = pltpu.get_barrier_semaphore()
        for c in range(4):
            pl.semaphore_signal(barrier, inc=1, device_id=self.goal(c, 1), device_id_type=MESH)

    def meet(self):
        pl.semaphore_wait(pltpu.get_barrier_semaphore(), 4)

    def coord(self, c, phase):
        return self.y if (c < 2) == (phase == 1) else self.z

    def rows(self, c, s):
        return pl.ds((c * self.subs + s) * self.height, self.height)

    def local(self, b, c, a, s):
        source = self.source(b)
        return source.at[:, a, self.rows(c, s), :] if c < 2 else source.at[a, :, self.rows(c, s), :]

    def chunk(self, c, phase, t):
        return self.wrap(self.coord(c, phase) - (1 - 2 * (c % 2)) * t)

    def copy1(self, b, c, t, s):
        src = self.recv1.at[b, c, t - 1, s] if t else self.local(b, c, self.chunk(c, 1, 1), s)
        dst = self.recv1.at[b, c, t, s]
        return pltpu.make_async_remote_copy(src, dst, self.s1.at[b, c, t, s], self.r1.at[b, c, t, s], device_id=self.goal(c, 1), device_id_type=MESH)

    def copy2(self, b, c, t, s):
        src = self.recv2.at[b, c, t - 1, s] if t else self.send2.at[b, c, s]
        dst = self.recv2.at[b, c, t, s]
        return pltpu.make_async_remote_copy(src, dst, self.s2.at[b, c, t, s], self.r2.at[b, c, t, s], device_id=self.goal(c, 2), device_id_type=MESH)

    def start(self, b):
        for s in range(self.subs):
            for c in range(4):
                self.copy1(b, c, 0, s).start()

    def hop1(self, b, t):
        for s in range(self.subs):
            for c in range(4):
                self.copy1(b, c, t, s).wait_recv()
                mine = self.local(b, c, self.chunk(c, 1, t + 2), s)[...]
                total = self.recv1[b, c, t, s].astype(F32) + mine.astype(F32)
                if t < self.n - 2:
                    self.recv1[b, c, t, s] = total.astype(BF16)
                    self.copy1(b, c, t + 1, s).start()
                else:
                    self.acc[b, c, s] = total
                    self.send2[b, c, s] = self.acc[b, c, s, self.chunk(c, 2, 1)].astype(BF16)
                    self.copy2(b, c, 0, s).start()

    def hop2(self, b, t, scale, store):
        for s in range(self.subs):
            for c in range(4):
                self.copy2(b, c, t, s).wait_recv()
                total = self.recv2[b, c, t, s].astype(F32) + self.acc[b, c, s, self.chunk(c, 2, t + 2)]
                if t < self.n - 2:
                    self.recv2[b, c, t, s] = total.astype(BF16)
                    self.copy2(b, c, t + 1, s).start()
                else:
                    store(b, (c * self.subs + s) * self.height, self.height, (total * scale).astype(BF16))

    def drain(self, b):
        for s in range(self.subs):
            for c in range(4):
                for t in range(self.n - 1):
                    self.copy1(b, c, t, s).wait_send()
                    self.copy2(b, c, t, s).wait_send()

    @staticmethod
    def scratch(n, blocks, subs, rows, width):
        height = rows // (4 * subs)
        return [
            pltpu.VMEM((blocks, 4, n - 1, subs, n, height, width), BF16),
            pltpu.VMEM((blocks, 4, subs, n, height, width), F32),
            pltpu.VMEM((blocks, 4, subs, height, width), BF16),
            pltpu.VMEM((blocks, 4, n - 1, subs, height, width), BF16),
        ] + [pltpu.SemaphoreType.DMA((blocks, 4, n - 1, subs))] * 4


def mlp_ring_kernel(n, subs, scale, blocks, slow, fast, m_ref, dy_ref, wg_ref, wu_ref, wd_ref, out_ref, grads_ref, act_ref, g_ref, *scratch):
    step = pl.program_id(0)
    seq, dim = m_ref.shape
    width = act_ref.shape[0]
    rows = dim // (n * n)
    tiles = 4
    blk, tile = seq // tiles, dim // tiles
    per_tile = tile // rows
    ring = Ring(n, subs, slow, fast, lambda b: g_ref.at[b], *scratch)
    at = lambda i, size: pl.ds(pl.multiple_of(i * size, size), size)

    @pl.when(step == 0)
    def _():
        ring.arrive()
        ring.meet()

    def store(b, first, height, value):
        out_ref[pl.ds(pl.multiple_of(b * 3 * width + first, height), height), :] = value

    hops = [functools.partial(ring.hop1, t=t) for t in range(n - 1)]
    hops += [functools.partial(ring.hop2, t=t, scale=scale, store=store) for t in range(n - 1)]
    slots = 2 * tiles
    delays = [3 * t + 4 if t < n - 1 else 3 * n + 2 * (t - n + 1) for t in range(2 * (n - 1))]

    def events(slot):
        for hop, delay in zip(hops, delays):
            since = slot - delay
            block = since // slots - 1

            @pl.when((since >= slots) & (lax.rem(since, slots) == 0) & (block < blocks))
            def _(hop=hop, block=block):
                hop(block)

    def forward(i):
        m, dy = m_ref[at(i, blk), :], dy_ref[at(i, blk), :]
        grad_act = nt(dy, wd_ref[...]).astype(BF16).astype(F32)
        act, grad_gate, grad_up = act_grads(nn(m, wg_ref[...]), nn(m, wu_ref[...]), grad_act)
        act_ref[:, at(i, blk)] = jnp.transpose(act)
        grads_ref[:width, at(i, blk)] = jnp.transpose(grad_gate)
        grads_ref[width:, at(i, blk)] = jnp.transpose(grad_up)

    def weights(i):
        grads = nn(grads_ref[...], m_ref[:, at(i, tile)]).astype(BF16)
        down = nn(act_ref[...], dy_ref[:, at(i, tile)]).astype(BF16)
        for k in range(per_tile):
            piece = i * per_tile + k
            g_ref[step, piece // n, lax.rem(piece, n), : 2 * width, :] = grads[:, k * rows : (k + 1) * rows]
            g_ref[step, piece // n, lax.rem(piece, n), 2 * width :, :] = down[:, k * rows : (k + 1) * rows]

    def slot_body(i, carry):
        @pl.when(i < tiles)
        def _():
            forward(i)

        @pl.when(i >= tiles)
        def _():
            weights(i - tiles)

        events(step * slots + i)
        return carry

    lax.fori_loop(0, slots, slot_body, 0)
    ring.start(step)

    @pl.when(step == blocks - 1)
    def _():
        def tail(slot, carry):
            events(slot)
            return carry

        lax.fori_loop(blocks * slots, (blocks + 1) * slots + max(delays), tail, 0)

        def drain(b, carry):
            ring.drain(b)
            return carry

        lax.fori_loop(0, blocks, drain, 0)


def mlp_ring(m, dy, w_gate, w_up, w_down, scale, slow, fast, n, collective_id):
    seq, dim = m.shape
    ff = w_gate.shape[1]
    width = min(256, ff)
    blocks = ff // width
    subs = 2
    rows = dim // (n * n)
    once = lambda shape: pl.BlockSpec(shape, lambda j: (0, 0), pipeline_mode=pl.Buffered(1))
    return pl.pallas_call(
        functools.partial(mlp_ring_kernel, n, subs, scale, blocks, slow, fast),
        grid=(blocks,),
        in_specs=[
            once((seq, dim)),
            once((seq, dim)),
            pl.BlockSpec((dim, width), lambda j: (0, j)),
            pl.BlockSpec((dim, width), lambda j: (0, j)),
            pl.BlockSpec((width, dim), lambda j: (j, 0)),
        ],
        out_specs=pl.BlockSpec((3 * ff, rows), lambda j: (0, 0)),
        scratch_shapes=[
            pltpu.VMEM((2 * width, seq), BF16),
            pltpu.VMEM((width, seq), BF16),
            pltpu.VMEM((blocks, n, n, 3 * width, rows), BF16),
        ]
        + Ring.scratch(n, blocks, subs, 3 * width, rows),
        out_shape=jax.ShapeDtypeStruct((3 * ff, rows), BF16),
        compiler_params=pltpu.CompilerParams(collective_id=collective_id, has_side_effects=True, vmem_limit_bytes=VMEM_LIMIT),
        cost_estimate=pl.CostEstimate(flops=18 * seq * dim * ff, bytes_accessed=4 * seq * dim, transcendentals=0),
        name="mlp_ring",
    )(m, dy, w_gate, w_up, w_down)


def ring_reduce_kernel(n, subs, scale, slow, fast, g_ref, out_ref, *scratch):
    ring = Ring(n, subs, slow, fast, lambda b: g_ref, *scratch)

    def store(b, first, height, value):
        out_ref[first : first + height, :] = value

    ring.arrive()
    ring.meet()
    ring.start(0)
    for t in range(n - 1):
        ring.hop1(0, t)
    for t in range(n - 1):
        ring.hop2(0, t, scale, store)
    ring.drain(0)


def ring_reduce(pieces, scale, subs, slow, fast, collective_id):
    total, rows, width = pieces.shape
    n = round(total**0.5)
    return pl.pallas_call(
        functools.partial(ring_reduce_kernel, n, subs, scale, slow, fast),
        out_shape=jax.ShapeDtypeStruct((rows, width), BF16),
        in_specs=[pl.BlockSpec(memory_space=pltpu.VMEM)],
        out_specs=pl.BlockSpec(memory_space=pltpu.VMEM),
        scratch_shapes=Ring.scratch(n, 1, subs, rows, width),
        compiler_params=pltpu.CompilerParams(collective_id=collective_id, has_side_effects=True, vmem_limit_bytes=VMEM_LIMIT),
        cost_estimate=pl.CostEstimate(flops=40_000_000_000, bytes_accessed=2 * total * rows * width, transcendentals=0),
        name="ring_reduce",
    )(pieces.reshape(n, n, rows, width))


def spread_mlp_kernel(groups, ff_local, width, in_ref, gate_ref, up_ref, down_ref):
    for g in range(groups):
        for at in range(g * ff_local, (g + 1) * ff_local, width):
            gate_ref[:, at : at + width] = jnp.transpose(in_ref[3 * at : 3 * at + width, :]).astype(F32)
            up_ref[:, at : at + width] = jnp.transpose(in_ref[3 * at + width : 3 * at + 2 * width, :]).astype(F32)
            down_ref[at : at + width, :] = in_ref[3 * at + 2 * width : 3 * at + 3 * width, :].astype(F32)


def spread_mlp(stacked, outer, groups, ff_local):
    total, rows = stacked.shape
    ff, dim = ff_local * groups, rows * outer
    return call(
        functools.partial(spread_mlp_kernel, groups, ff_local, min(256, ff_local)),
        total * rows,
        total * rows * 6,
        grid=(outer,),
        in_specs=[pl.BlockSpec((total // outer, rows), lambda o: (o, 0))],
        out_specs=[
            pl.BlockSpec((rows, ff), lambda o: (o, 0)),
            pl.BlockSpec((rows, ff), lambda o: (o, 0)),
            pl.BlockSpec((ff, rows), lambda o: (0, o)),
        ],
        out_shape=[jax.ShapeDtypeStruct((dim, ff), F32)] * 2 + [jax.ShapeDtypeStruct((ff, dim), F32)],
        name="spread_mlp",
    )(stacked)


def spread_attn_kernel(groups, q_width, k_width, in_ref, q_ref, k_ref, v_ref, o_ref, gain_ref):
    rows = q_ref.shape[0]
    gain = None
    for g in range(groups):
        piece = in_ref[g * rows : (g + 1) * rows, :].astype(F32)
        q_ref[:, g * q_width : (g + 1) * q_width] = piece[:, :q_width]
        k_ref[:, g * k_width : (g + 1) * k_width] = piece[:, q_width : q_width + k_width]
        v_ref[:, g * k_width : (g + 1) * k_width] = piece[:, q_width + k_width : q_width + 2 * k_width]
        o_ref[g * q_width : (g + 1) * q_width, :] = jnp.transpose(piece[:, q_width + 2 * k_width : 2 * (q_width + k_width)])
        part = piece[:8, 2 * (q_width + k_width) :]
        gain = part if gain is None else gain + part
    gain_ref[...] = gain


def spread_attn(stacked, outer, groups, q_width, k_width):
    total, row_width = stacked.shape
    rows = total // (outer * groups)
    dim = rows * outer
    return call(
        functools.partial(spread_attn_kernel, groups, q_width, k_width),
        total * row_width,
        total * row_width * 6,
        grid=(outer,),
        in_specs=[pl.BlockSpec((groups * rows, row_width), lambda o: (o, 0))],
        out_specs=[
            pl.BlockSpec((rows, groups * q_width), lambda o: (o, 0)),
            pl.BlockSpec((rows, groups * k_width), lambda o: (o, 0)),
            pl.BlockSpec((rows, groups * k_width), lambda o: (o, 0)),
            pl.BlockSpec((groups * q_width, rows), lambda o: (0, o)),
            pl.BlockSpec((8, rows), lambda o: (o, 0)),
        ],
        out_shape=[
            jax.ShapeDtypeStruct((dim, groups * q_width), F32),
            jax.ShapeDtypeStruct((dim, groups * k_width), F32),
            jax.ShapeDtypeStruct((dim, groups * k_width), F32),
            jax.ShapeDtypeStruct((groups * q_width, dim), F32),
            jax.ShapeDtypeStruct((8 * outer, rows), F32),
        ],
        name="spread_attn",
    )(stacked)


def solution(mesh):
    sp_size = mesh.shape["sp"]
    dp_size = mesh.shape["dp"]
    side = round(dp_size**0.5)
    grid = jax.sharding.Mesh(mesh.devices.reshape(side, dp_size // side, sp_size // 2, 2), ("z", "y", "x", "c"))
    seq_spec = P(("z", "y"), ("x", "c"), None)
    seq_axes, mlp_axes = ("x", "c"), ("y", "c")
    mlp_size = grid.shape["y"] * 2
    mlp_outer = grid.shape["z"] * grid.shape["x"]
    inv_batch = 1.0 / dp_size

    def device_step(tokens, grad_out, norm_attn, w_query, w_key, w_value, w_out, norm_mlp, w_gate, w_up, w_down):
        x = tokens[0]
        dy = grad_out[0]
        sp_idx = lax.axis_index(seq_axes)
        ff_idx = lax.axis_index(mlp_axes)
        n_local, dim = x.shape
        n_seq = n_local * sp_size
        q_width = w_query.shape[1] // sp_size
        k_width = w_key.shape[1] // sp_size
        ff_local = w_gate.shape[1] // mlp_size
        rows = dim // dp_size
        attn_blk = min(512, n_seq // 2)
        cos_all, sin_all = rope_tables(jnp.arange(n_seq))

        def to_heads(stacked):
            return lax.all_to_all(stacked, seq_axes, 0, 0, tiled=True)

        def gather(local, axes):
            return lax.all_gather(local, axes, axis=0, tiled=True)

        normed, unit_attn, inv_attn = norm_fwd(x, norm_attn)
        normed_full = gather(normed, seq_axes)
        dy_full = gather(dy, mlp_axes)
        qkv = qkv_heads(normed_full, w_query, w_key, w_value, cos_all, sin_all, sp_size, sp_idx)
        attn, lse = attn_fwd(qkv, attn_blk)
        attn_tok = to_heads(attn.reshape(sp_size, n_local, q_width))
        my_gate = lax.dynamic_slice_in_dim(w_gate, ff_idx * ff_local, ff_local, 1)
        my_up = lax.dynamic_slice_in_dim(w_up, ff_idx * ff_local, ff_local, 1)
        my_down = lax.dynamic_slice_in_dim(w_down, ff_idx * ff_local, ff_local, 0)
        w_out_heads = w_out.reshape(sp_size, q_width, dim)
        projected = jnp.einsum("jte,jed->td", attn_tok, w_out_heads, preferred_element_type=F32)
        hidden = (x.astype(F32) + projected).astype(BF16)
        normed_mlp, unit_mlp, inv_mlp = norm_fwd(hidden, norm_mlp)
        m_full = gather(normed_mlp, mlp_axes)

        grad_m = mlp_grad_input(normed_mlp, dy, w_gate, w_up, w_down, min(512, w_gate.shape[1]))
        grad_hid_norm, g_norm_mlp = norm_bwd(grad_m, unit_mlp, inv_mlp, norm_mlp)
        grad_hidden = (dy.astype(F32) + grad_hid_norm).astype(BF16)
        grad_hidden_full = gather(grad_hidden, seq_axes)

        g_mlp = mlp_ring(m_full, dy_full, my_gate, my_up, my_down, inv_batch, "z", "x", side, 1)
        g_mlp = gather(g_mlp, ("z", "x", "y", "c"))

        my_out = lax.dynamic_slice_in_dim(w_out, sp_idx * q_width, q_width, 0)
        grad_attn = nt(grad_hidden_full, my_out).astype(BF16)
        gqkv = attn_bwd(qkv, grad_attn, lse, cos_all, sin_all, attn_blk)
        gqkv_tok = to_heads(gqkv.reshape(sp_size, n_local, q_width + 2 * k_width))
        flat = lambda t: jnp.transpose(t, (1, 0, 2)).reshape(n_local, -1)
        grad_normed = (
            nt(flat(gqkv_tok[:, :, :q_width]), w_query)
            + nt(flat(gqkv_tok[:, :, q_width : q_width + k_width]), w_key)
            + nt(flat(gqkv_tok[:, :, q_width + k_width :]), w_value)
        ).astype(BF16)
        grad_tok_norm, g_norm_attn = norm_bwd(grad_normed, unit_attn, inv_attn, norm_attn)
        grad_tokens = (grad_hidden.astype(F32) + grad_tok_norm).astype(BF16)

        g_attn = jnp.concatenate([tn(normed_full, gqkv).astype(BF16), tn(grad_hidden_full, attn).astype(BF16)], axis=1)
        gains = jnp.stack([g_norm_attn.reshape(dp_size, rows), g_norm_mlp.reshape(dp_size, rows)], axis=1)
        gains = jnp.pad(gains.astype(BF16), ((0, 0), (0, rows - 2), (0, 0)))
        g_attn = jnp.concatenate([g_attn.reshape(dp_size, rows, 2 * (q_width + k_width)), gains], axis=2)
        g_attn = ring_reduce(g_attn, inv_batch, 2, "z", "y", 2)
        g_attn = gather(g_attn, ("z", "y", "x", "c"))

        g_gate, g_up, g_down = spread_mlp(g_mlp, mlp_outer, mlp_size, ff_local)
        g_query, g_key, g_value, g_out, gains = spread_attn(g_attn, dp_size, sp_size, q_width, k_width)
        gains = gains.reshape(dp_size, 8, rows)
        return (
            grad_tokens[None],
            gains[:, 0].reshape(dim),
            g_query,
            g_key,
            g_value,
            g_out,
            gains[:, 1].reshape(dim),
            g_gate,
            g_up,
            g_down,
        )

    return jax.shard_map(device_step, mesh=grid, in_specs=(seq_spec, seq_spec) + (P(),) * 9, out_specs=(seq_spec,) + (P(),) * 9, check_vma=False)
```

```python
import functools
import math

import jax
import jax.numpy as jnp
from jax import lax
from jax.experimental import pallas as pl
from jax.experimental.pallas import tpu as pltpu
from jax.sharding import PartitionSpec as P


NORM_EPS = 1.0e-5
ROPE_BASE = 1.0e6
HEAD_DIM = 128
F32 = jnp.float32
BF16 = jnp.bfloat16
VMEM_LIMIT = 60 * 1024 * 1024
MESH = pl.DeviceIdType.MESH
NEG = -1.0e30


def nn(a, b):
    return lax.dot_general(a, b, (((1,), (0,)), ((), ())), preferred_element_type=F32)


def nt(a, b):
    return lax.dot_general(a, b, (((1,), (1,)), ((), ())), preferred_element_type=F32)


def tn(a, b):
    return lax.dot_general(a, b, (((0,), (0,)), ((), ())), preferred_element_type=F32)


def norm_fwd(values, gain_vec):
    values_f = values.astype(F32)
    inv_rms = lax.rsqrt(jnp.mean(values_f * values_f, axis=-1, keepdims=True) + NORM_EPS)
    unit_vals = values_f * inv_rms
    return (unit_vals * gain_vec.astype(F32)).astype(BF16), unit_vals, inv_rms


def norm_bwd(grad_normed, unit_vals, inv_rms, gain_vec):
    grad_f = grad_normed.astype(F32)
    grad_gain = jnp.sum(grad_f * unit_vals, axis=0)
    grad_unit = grad_f * gain_vec.astype(F32)
    grad_in = inv_rms * (grad_unit - unit_vals * jnp.mean(grad_unit * unit_vals, axis=-1, keepdims=True))
    return grad_in, grad_gain


def rope_tables(positions):
    half_dim = HEAD_DIM // 2
    inv_freq = ROPE_BASE ** (-jnp.arange(half_dim, dtype=F32) * (2.0 / HEAD_DIM))
    angles = positions.astype(F32)[:, None] * inv_freq[None, :]
    cos, sin = jnp.cos(angles), jnp.sin(angles)
    return jnp.concatenate([cos, cos], axis=-1), jnp.concatenate([-sin, sin], axis=-1)


def rope(values, cos_tab, sin_tab):
    return values * cos_tab + pltpu.roll(values, HEAD_DIM // 2, 1) * sin_tab


def call(kernel, flops, moved, **kwargs):
    params = pltpu.CompilerParams(vmem_limit_bytes=VMEM_LIMIT)
    cost = pl.CostEstimate(flops=int(flops), bytes_accessed=int(moved), transcendentals=0)
    return pl.pallas_call(kernel, compiler_params=params, cost_estimate=cost, **kwargs)


def whole(shape):
    return pl.BlockSpec(shape, lambda *_: (0,) * len(shape))


def gather_qkv_kernel(x_ref, wq_ref, wk_ref, wv_ref, cos_blk, sin_blk, cos_row, sin_row, full_ref, qkv_ref, land, weights, w_sems, o_sems, i_send, i_recv, d_send, d_recv):
    x, c = lax.axis_index("x"), lax.axis_index("c")
    n = land.shape[0] // 2
    tok = x_ref.shape[0]
    half = tok // 2
    qw, kw = wq_ref.shape[1] // (2 * n), wk_ref.shape[1] // (2 * n)
    width = qw + 2 * kw
    wrap = lambda v: lax.rem(v + 2 * n, n)
    at = lambda dx, core: 2 * wrap(x + dx) + core
    me = 2 * x + c

    loads = []
    for k, (ref, start, size) in enumerate(((wq_ref, 0, qw), (wk_ref, qw, kw), (wv_ref, qw + kw, kw))):
        cols = pl.ds(pl.multiple_of(me * size, 128), size)
        loads.append(pltpu.make_async_copy(ref.at[:, cols], weights.at[:, pl.ds(start, size)], w_sems.at[k]))
        loads[-1].start()

    barrier = pltpu.get_barrier_semaphore()
    for goal in ({"x": wrap(x + 1)}, {"x": wrap(x - 1)}, {"c": 1 - c}):
        pl.semaphore_signal(barrier, inc=1, device_id=goal, device_id_type=MESH)
    pl.semaphore_wait(barrier, 3)

    rows = lambda h: pl.ds(h * half, half)

    def ring(way, hop, h):
        k = (0 if way > 0 else 3) + (h if hop == 0 else 2)
        src = land.at[at(-way * hop, c), rows(h)] if hop else x_ref.at[rows(h)]
        dst = land.at[at(-way * hop, c), rows(h)]
        return pltpu.make_async_remote_copy(src, dst, i_send.at[k], i_recv.at[k], device_id={"x": wrap(x + way)}, device_id_type=MESH)

    def across(k, dx, h):
        part = rows(h) if h is not None else pl.ds(0, tok)
        src = land.at[at(dx, c), part] if dx else x_ref.at[part]
        return pltpu.make_async_remote_copy(src, land.at[at(dx, c), part], d_send.at[k], d_recv.at[k], device_id={"c": 1 - c}, device_id_type=MESH)

    first = [ring(1, 0, 0), ring(-1, 0, 1), ring(1, 0, 1), ring(-1, 0, 0)]
    second = [ring(1, 1, 0), ring(-1, 1, 1)]
    die = [across(0, 0, None), across(1, -1, 0), across(2, 1, 1), across(3, -1, 1), across(4, 1, 0), across(5, 2, 0), across(6, 2, 1)]
    for copy in first[:2] + die[:1] + first[2:]:
        copy.start()
    land[me] = x_ref[...]
    for load in loads:
        load.wait()

    def wait_block(k):
        @pl.when(k == 1)
        def _():
            die[0].wait_recv()

        @pl.when(k == 2)
        def _():
            first[0].wait_recv()
            second[0].start()
            die[1].start()
            first[1].wait_recv()
            second[1].start()
            die[2].start()
            first[2].wait_recv()
            die[3].start()

        @pl.when(k == 3)
        def _():
            first[3].wait_recv()
            die[4].start()

        @pl.when(k == 4)
        def _():
            die[1].wait_recv()
            die[3].wait_recv()

        @pl.when(k == 5)
        def _():
            die[2].wait_recv()
            die[4].wait_recv()

        @pl.when(k == 6)
        def _():
            second[0].wait_recv()
            die[5].start()
            second[1].wait_recv()
            die[6].start()

        @pl.when(k == 7)
        def _():
            die[5].wait_recv()
            die[6].wait_recv()

    def out_copy(k):
        dx = jnp.where(k < 2, 0, jnp.where(k >= 6, 2, jnp.where(lax.rem(k, 2) == 0, -1, 1)))
        core = jnp.where((k == 1) | (k == 4) | (k == 5) | (k == 7), 1 - c, c)
        block = 2 * wrap(x + dx) + core
        here = pl.ds(pl.multiple_of(block * tok, tok), tok)
        return block, here, pltpu.make_async_copy(land.at[block], full_ref.at[here, :], o_sems.at[k])

    def body(k, carry):
        wait_block(k)
        block, here, copy = out_copy(k)
        copy.start()
        value = nn(land[block], weights[...])
        cos_b, sin_b = cos_blk[pl.ds(block, 1), :], sin_blk[pl.ds(block, 1), :]
        cos = cos_b * cos_row[...] - sin_b * sin_row[...]
        sin = sin_b * cos_row[...] + cos_b * sin_row[...]
        for start in range(0, width, HEAD_DIM):
            part = value[:, start : start + HEAD_DIM]
            if start < qw + kw:
                part = rope(part, cos, sin)
            qkv_ref[here, start : start + HEAD_DIM] = part.astype(BF16)
        return carry

    lax.fori_loop(0, 2 * n, body, 0)
    for copy in first + second + die:
        copy.wait_send()
    for k in range(2 * n):
        out_copy(k)[2].wait()


def gather_qkv(normed, w_query, w_key, w_value, groups, collective_id):
    tok, dim = normed.shape
    width = (w_query.shape[1] + w_key.shape[1] + w_value.shape[1]) // groups
    anywhere = pl.BlockSpec(memory_space=pl.ANY)
    vmem = pl.BlockSpec(memory_space=pltpu.VMEM)
    return pl.pallas_call(
        gather_qkv_kernel,
        in_specs=[vmem, anywhere, anywhere, anywhere, vmem, vmem, vmem, vmem],
        out_specs=[anywhere, vmem],
        out_shape=[jax.ShapeDtypeStruct((groups * tok, dim), BF16), jax.ShapeDtypeStruct((groups * tok, width), BF16)],
        scratch_shapes=[
            pltpu.VMEM((groups, tok, dim), BF16),
            pltpu.VMEM((dim, width), BF16),
            pltpu.SemaphoreType.DMA((3,)),
            pltpu.SemaphoreType.DMA((groups,)),
            pltpu.SemaphoreType.DMA((6,)),
            pltpu.SemaphoreType.DMA((6,)),
            pltpu.SemaphoreType.DMA((7,)),
            pltpu.SemaphoreType.DMA((7,)),
        ],
        compiler_params=pltpu.CompilerParams(collective_id=collective_id, has_side_effects=True, vmem_limit_bytes=VMEM_LIMIT),
        cost_estimate=pl.CostEstimate(flops=20_000_000_000, bytes_accessed=6 * groups * tok * dim, transcendentals=0),
        name="gather_qkv",
    )(normed, w_query, w_key, w_value, *rope_tables(jnp.arange(groups) * tok), *rope_tables(jnp.arange(tok)))


def attn_fwd_kernel(blk, n_q, qkv_ref, out_ref, lse_ref, tok_ref, mine, land, send_sems, recv_sems, *scrs):
    step, steps = pl.program_id(0), pl.num_programs(0)
    x, c = lax.axis_index("x"), lax.axis_index("c")
    me = 2 * x + c
    tok = blk // 2

    def block_of(step):
        ahead = jnp.where(step == 0, 2, jnp.where(step == 1, 1, jnp.where(step == 2, steps - 1, 0)))
        return lax.rem(x + ahead, steps)

    def send(step, core):
        goal = block_of(step)
        src = mine.at[2 * goal + core]
        return pltpu.make_async_remote_copy(src, land.at[me], send_sems.at[step, core], recv_sems.at[me], device_id={"x": goal, "c": core}, device_id_type=MESH)

    @pl.when(step == 0)
    def _():
        barrier = pltpu.get_barrier_semaphore()
        for k in range(1, 2 * steps):
            peer = lax.rem(me + k, 2 * steps)
            pl.semaphore_signal(barrier, inc=1, device_id={"x": peer // 2, "c": lax.rem(peer, 2)}, device_id_type=MESH)
        pl.semaphore_wait(barrier, 2 * steps - 1)

    @pl.when(step > 0)
    def _():
        send(step - 1, 0).start()
        send(step - 1, 1).start()

    i = block_of(step)
    coef = HEAD_DIM**-0.5 * math.log2(math.e)
    k_at, v_at = n_q * HEAD_DIM, (n_q + 1) * HEAD_DIM
    at = lambda j: pl.ds(pl.multiple_of(j * blk, blk), blk)
    lanes = lambda t, op: functools.reduce(op, [t[:, s : s + 128] for s in range(0, blk, 128)])
    qs = [qkv_ref[at(i), h * HEAD_DIM : (h + 1) * HEAD_DIM] for h in range(n_q)]
    causal = lax.broadcasted_iota(jnp.int32, (blk, blk), 0) >= lax.broadcasted_iota(jnp.int32, (blk, blk), 1)

    def score_step(j, tops, masked):
        key = qkv_ref[at(j), k_at:v_at]
        new = []
        for h in range(n_q):
            s = nt(qs[h], key)
            if masked:
                s = jnp.where(causal, s, NEG)
            scrs[h][:, at(j)] = s
            new.append(jnp.maximum(tops[h], lanes(s, jnp.maximum)))
        return tuple(new)

    start = tuple(jnp.full((blk, 128), NEG, F32) for _ in range(n_q))
    tops = lax.fori_loop(0, i, lambda j, t: score_step(j, t, False), start)
    tops = score_step(i, tops, True)
    row_max = [jnp.max(t, axis=1, keepdims=True) for t in tops]

    def exp_step(j, sums):
        new = []
        for h in range(n_q):
            e = jnp.exp2((scrs[h][:, at(j)] - row_max[h]) * coef)
            scrs[h][:, at(j)] = e
            new.append(sums[h] + lanes(e, jnp.add))
        return tuple(new)

    sums = lax.fori_loop(0, i + 1, exp_step, tuple(jnp.zeros((blk, 128), F32) for _ in range(n_q)))
    row_sum = [jnp.sum(t, axis=1, keepdims=True) for t in sums]
    inv_sum = [1.0 / t for t in row_sum]

    def out_step(j, accs):
        value = qkv_ref[at(j), v_at : v_at + HEAD_DIM]
        return tuple(accs[h] + nn((scrs[h][:, at(j)] * inv_sum[h]).astype(BF16), value) for h in range(n_q))

    accs = lax.fori_loop(0, i + 1, out_step, tuple(jnp.zeros((blk, HEAD_DIM), F32) for _ in range(n_q)))
    for h in range(n_q):
        value = accs[h].astype(BF16)
        out_ref[at(i), h * HEAD_DIM : (h + 1) * HEAD_DIM] = value
        for core in range(2):
            mine[2 * i + core, :, h * HEAD_DIM : (h + 1) * HEAD_DIM] = value[core * tok : (core + 1) * tok, :]
        log_norm = row_max[h] * coef + jnp.log2(row_sum[h])
        lse_ref[h * 8 : (h + 1) * 8, at(i)] = jnp.transpose(jnp.broadcast_to(log_norm, (blk, 128)))[:8, :]

    @pl.when(step == steps - 1)
    def _():
        land[me] = mine[me]
        send(step, 1 - c).start()
        for k in range(1, 2 * steps):
            peer = lax.rem(me + k, 2 * steps)
            pltpu.make_async_remote_copy(mine.at[peer], land.at[peer], send_sems.at[0, 0], recv_sems.at[peer], device_id={"x": x, "c": c}, device_id_type=MESH).wait_recv()
        tok_ref[...] = land[...]
        for k in range(steps - 1):
            send(k, 0).wait_send()
            send(k, 1).wait_send()
        send(step, 1 - c).wait_send()


def attn_fwd(qkv, steps, collective_id):
    seq, width = qkv.shape
    n_q = width // HEAD_DIM - 2
    blk = seq // steps
    return pl.pallas_call(
        functools.partial(attn_fwd_kernel, blk, n_q),
        grid=(steps,),
        in_specs=[whole((seq, width))],
        out_specs=[whole((seq, n_q * HEAD_DIM)), whole((8 * n_q, seq)), whole((2 * steps, blk // 2, n_q * HEAD_DIM))],
        out_shape=[
            jax.ShapeDtypeStruct((seq, n_q * HEAD_DIM), BF16),
            jax.ShapeDtypeStruct((8 * n_q, seq), F32),
            jax.ShapeDtypeStruct((2 * steps, blk // 2, n_q * HEAD_DIM), BF16),
        ],
        scratch_shapes=[pltpu.VMEM((2 * steps, blk // 2, n_q * HEAD_DIM), BF16)] * 2
        + [pltpu.SemaphoreType.DMA((steps, 2)), pltpu.SemaphoreType.DMA((2 * steps,))]
        + [pltpu.VMEM((blk, seq), F32)] * n_q,
        compiler_params=pltpu.CompilerParams(collective_id=collective_id, has_side_effects=True, vmem_limit_bytes=VMEM_LIMIT),
        cost_estimate=pl.CostEstimate(flops=2 * n_q * seq * seq * HEAD_DIM * 2, bytes_accessed=seq * width * 2, transcendentals=0),
        name="attn_fwd",
    )(qkv)


def attn_bwd_kernel(blk, n_q, qkv_ref, do_ref, lse_ref, cos_ref, sin_ref, out_ref, dk_scr, dv_scr, *scrs):
    i, steps = pl.program_id(0), pl.num_programs(0)
    scale = HEAD_DIM**-0.5
    coef = scale * math.log2(math.e)
    k_at, v_at = n_q * HEAD_DIM, (n_q + 1) * HEAD_DIM
    at = lambda j: pl.ds(pl.multiple_of(j * blk, blk), blk)
    p_scrs, dp_scrs = scrs[:n_q], scrs[n_q:]
    qs = [qkv_ref[at(i), h * HEAD_DIM : (h + 1) * HEAD_DIM] for h in range(n_q)]
    dos = [do_ref[:, h * HEAD_DIM : (h + 1) * HEAD_DIM] for h in range(n_q)]
    lses = [lse_ref[h * 8 : h * 8 + 1, :] for h in range(n_q)]
    causal = lax.broadcasted_iota(jnp.int32, (blk, blk), 0) <= lax.broadcasted_iota(jnp.int32, (blk, blk), 1)

    @pl.when(i == 0)
    def _():
        dk_scr[...] = jnp.zeros_like(dk_scr)
        dv_scr[...] = jnp.zeros_like(dv_scr)

    def prob_step(j, dots, masked):
        key, value = qkv_ref[at(j), k_at:v_at], qkv_ref[at(j), v_at : v_at + HEAD_DIM]
        new, dv = [], dv_scr[at(j), :]
        for h in range(n_q):
            p = jnp.exp2(nt(key, qs[h]) * coef - lses[h])
            if masked:
                p = jnp.where(causal, p, 0.0)
            dp = nt(value, dos[h]).astype(BF16)
            p_scrs[h][at(j), :] = p
            dp_scrs[h][at(j), :] = dp
            dv = dv + nn(p.astype(BF16), dos[h])
            new.append(dots[h] + jnp.sum((p * dp.astype(F32)).reshape(blk // 8, 8, blk), axis=0))
        dv_scr[at(j), :] = dv
        return tuple(new)

    dots = lax.fori_loop(0, i, lambda j, t: prob_step(j, t, False), tuple(jnp.zeros((8, blk), F32) for _ in range(n_q)))
    dots = prob_step(i, dots, True)
    row_dot = [jnp.sum(t, axis=0, keepdims=True) for t in dots]

    def grad_step(j, accs):
        key = qkv_ref[at(j), k_at:v_at]
        new, dk = [], dk_scr[at(j), :]
        for h in range(n_q):
            ds = (p_scrs[h][at(j), :] * (dp_scrs[h][at(j), :].astype(F32) - row_dot[h]) * scale).astype(BF16)
            dk = dk + nn(ds, qs[h])
            new.append(accs[h] + tn(ds, key))
        dk_scr[at(j), :] = dk
        return tuple(new)

    accs = lax.fori_loop(0, i + 1, grad_step, tuple(jnp.zeros((blk, HEAD_DIM), F32) for _ in range(n_q)))
    unrope = lambda g, sl: rope(g.astype(BF16).astype(F32), cos_ref[sl, :], -sin_ref[sl, :]).astype(BF16)
    for h in range(n_q):
        out_ref[at(i), h * HEAD_DIM : (h + 1) * HEAD_DIM] = unrope(accs[h], at(i))

    @pl.when(i == steps - 1)
    def _():
        def finish(j, carry):
            out_ref[at(j), k_at:v_at] = unrope(dk_scr[at(j), :], at(j))
            out_ref[at(j), v_at : v_at + HEAD_DIM] = dv_scr[at(j), :].astype(BF16)
            return carry

        lax.fori_loop(0, steps, finish, 0)


def attn_bwd(qkv, grad_out, lse, cos, sin, blk):
    seq, width = qkv.shape
    n_q = width // HEAD_DIM - 2
    return call(
        functools.partial(attn_bwd_kernel, blk, n_q),
        5 * n_q * seq * seq * HEAD_DIM * 2,
        seq * width * 4,
        grid=(seq // blk,),
        in_specs=[
            whole((seq, width)),
            pl.BlockSpec((blk, n_q * HEAD_DIM), lambda i: (i, 0)),
            pl.BlockSpec((8 * n_q, blk), lambda i: (0, i)),
            whole((seq, HEAD_DIM)),
            whole((seq, HEAD_DIM)),
        ],
        out_specs=whole((seq, width)),
        out_shape=jax.ShapeDtypeStruct((seq, width), BF16),
        scratch_shapes=[pltpu.VMEM((seq, HEAD_DIM), F32)] * 2
        + [pltpu.VMEM((seq, blk), F32)] * n_q
        + [pltpu.VMEM((seq, blk), BF16)] * n_q,
        name="attn_bwd",
    )(qkv, grad_out, lse, cos, sin)


def act_grads(gate, up, grad_act):
    sig = 1.0 / (1.0 + jnp.exp(-gate))
    act = gate * sig
    grad_gate = (grad_act * up * sig * (1.0 + gate * (1.0 - sig))).astype(BF16)
    grad_up = (grad_act * act).astype(BF16)
    return (act * up).astype(BF16), grad_gate, grad_up


def mlp_kernel(m_ref, dy_ref, wg_ref, wu_ref, wd_ref, out_ref, acc_ref):
    step = pl.program_id(0)
    m, dy = m_ref[...], dy_ref[...]
    grad_act = nt(dy, wd_ref[...]).astype(BF16).astype(F32)
    _, grad_gate, grad_up = act_grads(nn(m, wg_ref[...]), nn(m, wu_ref[...]), grad_act)
    total = nt(grad_gate, wg_ref[...]) + nt(grad_up, wu_ref[...])

    @pl.when(step == 0)
    def _():
        acc_ref[...] = total

    @pl.when(step > 0)
    def _():
        acc_ref[...] += total

    @pl.when(step == pl.num_programs(0) - 1)
    def _():
        out_ref[...] = acc_ref[...].astype(BF16)


def mlp_grad_input(m, dy, w_gate, w_up, w_down, blk):
    tok, dim = m.shape
    width = w_gate.shape[1]
    return call(
        mlp_kernel,
        5 * 2 * tok * dim * width,
        3 * 2 * dim * width,
        grid=(width // blk,),
        in_specs=[
            whole((tok, dim)),
            whole((tok, dim)),
            pl.BlockSpec((dim, blk), lambda j: (0, j)),
            pl.BlockSpec((dim, blk), lambda j: (0, j)),
            pl.BlockSpec((blk, dim), lambda j: (j, 0)),
        ],
        out_specs=whole((tok, dim)),
        out_shape=jax.ShapeDtypeStruct((tok, dim), BF16),
        scratch_shapes=[pltpu.VMEM((tok, dim), F32)],
        name="mlp_grad_input",
    )(m, dy, w_gate, w_up, w_down)


class Ring:
    def __init__(self, n, subs, slow, fast, source, recv1, acc, send2, recv2, s1, r1, s2, r2):
        self.n, self.subs, self.slow, self.fast, self.source = n, subs, slow, fast, source
        self.recv1, self.acc, self.send2, self.recv2 = recv1, acc, send2, recv2
        self.s1, self.r1, self.s2, self.r2 = s1, r1, s2, r2
        self.z, self.y = lax.axis_index(slow), lax.axis_index(fast)
        self.height = recv1.shape[5]

    def wrap(self, v):
        return lax.rem(v + 2 * self.n, self.n)

    def goal(self, c, phase):
        step = 1 - 2 * (c % 2)
        if (c < 2) == (phase == 1):
            return {self.fast: self.wrap(self.y + step)}
        return {self.slow: self.wrap(self.z + step)}

    def arrive(self):
        barrier = pltpu.get_barrier_semaphore()
        for c in range(4):
            pl.semaphore_signal(barrier, inc=1, device_id=self.goal(c, 1), device_id_type=MESH)

    def meet(self):
        pl.semaphore_wait(pltpu.get_barrier_semaphore(), 4)

    def coord(self, c, phase):
        return self.y if (c < 2) == (phase == 1) else self.z

    def rows(self, c, s):
        return pl.ds((c * self.subs + s) * self.height, self.height)

    def local(self, b, c, a, s):
        source = self.source(b)
        return source.at[:, a, self.rows(c, s), :] if c < 2 else source.at[a, :, self.rows(c, s), :]

    def chunk(self, c, phase, t):
        return self.wrap(self.coord(c, phase) - (1 - 2 * (c % 2)) * t)

    def copy1(self, b, c, t, s):
        src = self.recv1.at[b, c, t - 1, s] if t else self.local(b, c, self.chunk(c, 1, 1), s)
        dst = self.recv1.at[b, c, t, s]
        return pltpu.make_async_remote_copy(src, dst, self.s1.at[b, c, t, s], self.r1.at[b, c, t, s], device_id=self.goal(c, 1), device_id_type=MESH)

    def copy2(self, b, c, t, s):
        src = self.recv2.at[b, c, t - 1, s] if t else self.send2.at[b, c, s]
        dst = self.recv2.at[b, c, t, s]
        return pltpu.make_async_remote_copy(src, dst, self.s2.at[b, c, t, s], self.r2.at[b, c, t, s], device_id=self.goal(c, 2), device_id_type=MESH)

    def start(self, b):
        for s in range(self.subs):
            for c in range(4):
                self.copy1(b, c, 0, s).start()

    def hop1(self, b, t):
        for s in range(self.subs):
            for c in range(4):
                self.copy1(b, c, t, s).wait_recv()
                mine = self.local(b, c, self.chunk(c, 1, t + 2), s)[...]
                total = self.recv1[b, c, t, s].astype(F32) + mine.astype(F32)
                if t < self.n - 2:
                    self.recv1[b, c, t, s] = total.astype(BF16)
                    self.copy1(b, c, t + 1, s).start()
                else:
                    self.acc[b, c, s] = total
                    self.send2[b, c, s] = self.acc[b, c, s, self.chunk(c, 2, 1)].astype(BF16)
                    self.copy2(b, c, 0, s).start()

    def hop2(self, b, t, scale, store):
        for s in range(self.subs):
            for c in range(4):
                self.copy2(b, c, t, s).wait_recv()
                total = self.recv2[b, c, t, s].astype(F32) + self.acc[b, c, s, self.chunk(c, 2, t + 2)]
                if t < self.n - 2:
                    self.recv2[b, c, t, s] = total.astype(BF16)
                    self.copy2(b, c, t + 1, s).start()
                else:
                    store(b, (c * self.subs + s) * self.height, self.height, (total * scale).astype(BF16))

    def drain(self, b):
        for s in range(self.subs):
            for c in range(4):
                for t in range(self.n - 1):
                    self.copy1(b, c, t, s).wait_send()
                    self.copy2(b, c, t, s).wait_send()

    @staticmethod
    def scratch(n, blocks, subs, rows, width):
        height = rows // (4 * subs)
        return [
            pltpu.VMEM((blocks, 4, n - 1, subs, n, height, width), BF16),
            pltpu.VMEM((blocks, 4, subs, n, height, width), F32),
            pltpu.VMEM((blocks, 4, subs, height, width), BF16),
            pltpu.VMEM((blocks, 4, n - 1, subs, height, width), BF16),
        ] + [pltpu.SemaphoreType.DMA((blocks, 4, n - 1, subs))] * 4


def mlp_ring_kernel(n, subs, scale, blocks, slow, fast, group, m_ref, dy_ref, wg_all, wu_all, wd_all, out_ref, wg_buf, wu_buf, wd_buf, w_sems, grads_ref, act_ref, g_ref, *scratch):
    step = pl.program_id(0)
    seq, dim = m_ref.shape
    width = act_ref.shape[0]
    rows = dim // (n * n)
    tiles = 4
    blk, tile = seq // tiles, dim // tiles
    per_tile = tile // rows
    ring = Ring(n, subs, slow, fast, lambda b: g_ref.at[b], *scratch)
    at = lambda i, size: pl.ds(pl.multiple_of(i * size, size), size)

    def loads(b):
        mine = at((lax.axis_index(group) if group else 0) * blocks + b, width)
        slot = lax.rem(b, 2)
        return [
            pltpu.make_async_copy(wg_all.at[:, mine], wg_buf.at[slot], w_sems.at[slot, 0]),
            pltpu.make_async_copy(wu_all.at[:, mine], wu_buf.at[slot], w_sems.at[slot, 1]),
            pltpu.make_async_copy(wd_all.at[mine, :], wd_buf.at[slot], w_sems.at[slot, 2]),
        ]

    @pl.when(step == 0)
    def _():
        for load in loads(0):
            load.start()
        ring.arrive()
        ring.meet()

    @pl.when(step + 1 < blocks)
    def _():
        for load in loads(step + 1):
            load.start()

    for load in loads(step):
        load.wait()
    wg_ref, wu_ref, wd_ref = (buf.at[lax.rem(step, 2)] for buf in (wg_buf, wu_buf, wd_buf))

    def store(b, first, height, value):
        out_ref[pl.ds(pl.multiple_of(b * 3 * width + first, height), height), :] = value

    hops = [functools.partial(ring.hop1, t=t) for t in range(n - 1)]
    hops += [functools.partial(ring.hop2, t=t, scale=scale, store=store) for t in range(n - 1)]
    slots = 2 * tiles
    delays = [3 * t + 4 if t < n - 1 else 3 * n + 2 * (t - n + 1) for t in range(2 * (n - 1))]

    def events(slot):
        for hop, delay in zip(hops, delays):
            since = slot - delay
            block = since // slots - 1

            @pl.when((since >= slots) & (lax.rem(since, slots) == 0) & (block < blocks))
            def _(hop=hop, block=block):
                hop(block)

    def forward(i):
        m, dy = m_ref[at(i, blk), :], dy_ref[at(i, blk), :]
        grad_act = nt(dy, wd_ref[...]).astype(BF16).astype(F32)
        act, grad_gate, grad_up = act_grads(nn(m, wg_ref[...]), nn(m, wu_ref[...]), grad_act)
        act_ref[:, at(i, blk)] = jnp.transpose(act)
        grads_ref[:width, at(i, blk)] = jnp.transpose(grad_gate)
        grads_ref[width:, at(i, blk)] = jnp.transpose(grad_up)

    def weights(i):
        grads = nn(grads_ref[...], m_ref[:, at(i, tile)]).astype(BF16)
        down = nn(act_ref[...], dy_ref[:, at(i, tile)]).astype(BF16)
        for k in range(per_tile):
            piece = i * per_tile + k
            g_ref[step, piece // n, lax.rem(piece, n), : 2 * width, :] = grads[:, k * rows : (k + 1) * rows]
            g_ref[step, piece // n, lax.rem(piece, n), 2 * width :, :] = down[:, k * rows : (k + 1) * rows]

    def slot_body(i, carry):
        @pl.when(i < tiles)
        def _():
            forward(i)

        @pl.when(i >= tiles)
        def _():
            weights(i - tiles)

        events(step * slots + i)
        return carry

    lax.fori_loop(0, slots, slot_body, 0)
    ring.start(step)

    @pl.when(step == blocks - 1)
    def _():
        def tail(slot, carry):
            events(slot)
            return carry

        lax.fori_loop(blocks * slots, (blocks + 1) * slots + max(delays), tail, 0)

        def drain(b, carry):
            ring.drain(b)
            return carry

        lax.fori_loop(0, blocks, drain, 0)


def mlp_ring(m, dy, w_gate, w_up, w_down, ff, scale, slow, fast, n, group, collective_id):
    seq, dim = m.shape
    width = min(256, ff)
    blocks = ff // width
    subs = 2
    rows = dim // (n * n)
    once = lambda shape: pl.BlockSpec(shape, lambda j: (0, 0), pipeline_mode=pl.Buffered(1))
    anywhere = pl.BlockSpec(memory_space=pl.ANY)
    return pl.pallas_call(
        functools.partial(mlp_ring_kernel, n, subs, scale, blocks, slow, fast, group),
        grid=(blocks,),
        in_specs=[once((seq, dim)), once((seq, dim)), anywhere, anywhere, anywhere],
        out_specs=pl.BlockSpec((3 * ff, rows), lambda j: (0, 0)),
        scratch_shapes=[
            pltpu.VMEM((2, dim, width), BF16),
            pltpu.VMEM((2, dim, width), BF16),
            pltpu.VMEM((2, width, dim), BF16),
            pltpu.SemaphoreType.DMA((2, 3)),
            pltpu.VMEM((2 * width, seq), BF16),
            pltpu.VMEM((width, seq), BF16),
            pltpu.VMEM((blocks, n, n, 3 * width, rows), BF16),
        ]
        + Ring.scratch(n, blocks, subs, 3 * width, rows),
        out_shape=jax.ShapeDtypeStruct((3 * ff, rows), BF16),
        compiler_params=pltpu.CompilerParams(collective_id=collective_id, has_side_effects=True, vmem_limit_bytes=VMEM_LIMIT),
        cost_estimate=pl.CostEstimate(flops=18 * seq * dim * ff, bytes_accessed=4 * seq * dim, transcendentals=0),
        name="mlp_ring",
    )(m, dy, w_gate, w_up, w_down)


def ring_reduce_kernel(n, subs, scale, slow, fast, g_ref, out_ref, *scratch):
    ring = Ring(n, subs, slow, fast, lambda b: g_ref, *scratch)

    def store(b, first, height, value):
        out_ref[first : first + height, :] = value

    ring.arrive()
    ring.meet()
    ring.start(0)
    for t in range(n - 1):
        ring.hop1(0, t)
    for t in range(n - 1):
        ring.hop2(0, t, scale, store)
    ring.drain(0)


def ring_reduce(pieces, scale, subs, slow, fast, collective_id):
    total, rows, width = pieces.shape
    n = round(total**0.5)
    return pl.pallas_call(
        functools.partial(ring_reduce_kernel, n, subs, scale, slow, fast),
        out_shape=jax.ShapeDtypeStruct((rows, width), BF16),
        in_specs=[pl.BlockSpec(memory_space=pltpu.VMEM)],
        out_specs=pl.BlockSpec(memory_space=pltpu.VMEM),
        scratch_shapes=Ring.scratch(n, 1, subs, rows, width),
        compiler_params=pltpu.CompilerParams(collective_id=collective_id, has_side_effects=True, vmem_limit_bytes=VMEM_LIMIT),
        cost_estimate=pl.CostEstimate(flops=40_000_000_000, bytes_accessed=2 * total * rows * width, transcendentals=0),
        name="ring_reduce",
    )(pieces.reshape(n, n, rows, width))


def spread_mlp_kernel(groups, ff_local, width, in_ref, gate_ref, up_ref, down_ref):
    for g in range(groups):
        for at in range(g * ff_local, (g + 1) * ff_local, width):
            gate_ref[:, at : at + width] = jnp.transpose(in_ref[3 * at : 3 * at + width, :]).astype(F32)
            up_ref[:, at : at + width] = jnp.transpose(in_ref[3 * at + width : 3 * at + 2 * width, :]).astype(F32)
            down_ref[at : at + width, :] = in_ref[3 * at + 2 * width : 3 * at + 3 * width, :].astype(F32)


def spread_mlp(stacked, outer, groups, ff_local):
    total, rows = stacked.shape
    ff, dim = ff_local * groups, rows * outer
    return call(
        functools.partial(spread_mlp_kernel, groups, ff_local, min(256, ff_local)),
        total * rows,
        total * rows * 6,
        grid=(outer,),
        in_specs=[pl.BlockSpec((total // outer, rows), lambda o: (o, 0))],
        out_specs=[
            pl.BlockSpec((rows, ff), lambda o: (o, 0)),
            pl.BlockSpec((rows, ff), lambda o: (o, 0)),
            pl.BlockSpec((ff, rows), lambda o: (0, o)),
        ],
        out_shape=[jax.ShapeDtypeStruct((dim, ff), F32)] * 2 + [jax.ShapeDtypeStruct((ff, dim), F32)],
        name="spread_mlp",
    )(stacked)


def spread_attn_kernel(groups, q_width, k_width, in_ref, q_ref, k_ref, v_ref, o_ref, gain_ref):
    rows = q_ref.shape[0]
    gain = None
    for g in range(groups):
        piece = in_ref[g * rows : (g + 1) * rows, :].astype(F32)
        q_ref[:, g * q_width : (g + 1) * q_width] = piece[:, :q_width]
        k_ref[:, g * k_width : (g + 1) * k_width] = piece[:, q_width : q_width + k_width]
        v_ref[:, g * k_width : (g + 1) * k_width] = piece[:, q_width + k_width : q_width + 2 * k_width]
        gain_at, o_at = q_width + 2 * k_width, q_width + 2 * k_width + rows
        block, core = g // 2, g % 2
        o_ref[core * q_width : (core + 1) * q_width, block * rows : (block + 1) * rows] = jnp.transpose(piece[:, o_at:])
        part = piece[:8, gain_at:o_at]
        gain = part if gain is None else gain + part
    gain_ref[...] = gain


def spread_attn(stacked, nz, ny, groups, q_width, k_width):
    total, row_width = stacked.shape
    outer = nz * ny
    rows = total // (outer * groups)
    dim = rows * outer
    nx = groups // 2
    return call(
        functools.partial(spread_attn_kernel, groups, q_width, k_width),
        total * row_width,
        total * row_width * 6,
        grid=(outer,),
        in_specs=[pl.BlockSpec((groups * rows, row_width), lambda o: (o, 0))],
        out_specs=[
            pl.BlockSpec((rows, groups * q_width), lambda o: (o, 0)),
            pl.BlockSpec((rows, groups * k_width), lambda o: (o, 0)),
            pl.BlockSpec((rows, groups * k_width), lambda o: (o, 0)),
            pl.BlockSpec((2 * q_width, nx * rows), lambda o: (o % ny, o // ny)),
            pl.BlockSpec((8, rows), lambda o: (o, 0)),
        ],
        out_shape=[
            jax.ShapeDtypeStruct((dim, groups * q_width), F32),
            jax.ShapeDtypeStruct((dim, groups * k_width), F32),
            jax.ShapeDtypeStruct((dim, groups * k_width), F32),
            jax.ShapeDtypeStruct((2 * ny * q_width, nz * nx * rows), F32),
            jax.ShapeDtypeStruct((8 * outer, rows), F32),
        ],
        name="spread_attn",
    )(stacked)


def solution(mesh):
    sp_size = mesh.shape["sp"]
    dp_size = mesh.shape["dp"]
    side = round(dp_size**0.5)
    grid = jax.sharding.Mesh(mesh.devices.reshape(side, dp_size // side, sp_size // 2, 2), ("z", "y", "x", "c"))
    seq_spec = P(("z", "y"), ("x", "c"), None)
    seq_axes, mlp_axes = ("x", "c"), ("y", "c")
    mlp_size = grid.shape["y"] * 2
    mlp_outer = grid.shape["z"] * grid.shape["x"]
    inv_batch = 1.0 / dp_size

    def device_step(tokens, grad_out, norm_attn, w_query, w_key, w_value, w_out, norm_mlp, w_gate, w_up, w_down):
        x = tokens[0]
        dy = grad_out[0]
        n_local, dim = x.shape
        n_seq = n_local * sp_size
        q_width = w_query.shape[1] // sp_size
        k_width = w_key.shape[1] // sp_size
        ff_local = w_gate.shape[1] // mlp_size
        rows = dim // dp_size
        attn_blk = min(512, n_seq // 2)
        cos_all, sin_all = rope_tables(jnp.arange(n_seq))

        def to_heads(stacked):
            return lax.all_to_all(stacked, seq_axes, 0, 0, tiled=True)

        def gather(local, axes):
            return lax.all_gather(local, axes, axis=0, tiled=True)

        normed, unit_attn, inv_attn = norm_fwd(x, norm_attn)
        dy_full = gather(dy, mlp_axes)
        normed_full, qkv = gather_qkv(normed, w_query, w_key, w_value, sp_size, 3)
        _, lse, attn_tok = attn_fwd(qkv, sp_size // 2, 4)
        w_out_heads = w_out.reshape(sp_size, q_width, dim)
        projected = jnp.einsum("jte,jed->td", attn_tok, w_out_heads, preferred_element_type=F32)
        hidden = (x.astype(F32) + projected).astype(BF16)
        normed_mlp, unit_mlp, inv_mlp = norm_fwd(hidden, norm_mlp)
        m_full = gather(normed_mlp, mlp_axes)

        grad_m = mlp_grad_input(normed_mlp, dy, w_gate, w_up, w_down, min(512, w_gate.shape[1]))
        grad_hid_norm, g_norm_mlp = norm_bwd(grad_m, unit_mlp, inv_mlp, norm_mlp)
        grad_hidden = (dy.astype(F32) + grad_hid_norm).astype(BF16)
        grad_hidden_y = gather(grad_hidden, mlp_axes)
        attn_y = lax.all_to_all(attn_tok, mlp_axes, 0, 0, tiled=True).reshape(n_seq, q_width)

        g_mlp = mlp_ring(m_full, dy_full, w_gate, w_up, w_down, ff_local, inv_batch, "z", "x", side, mlp_axes, 1)
        g_mlp, late_hidden = lax.optimization_barrier((g_mlp, grad_hidden))
        g_mlp = gather(g_mlp, ("z", "x", "y", "c"))

        grad_attn = jnp.einsum("td,jed->jte", late_hidden, w_out_heads, preferred_element_type=F32).astype(BF16)
        grad_attn = to_heads(grad_attn).reshape(n_seq, q_width)
        g_out = tn(grad_hidden_y, attn_y).astype(BF16).reshape(mlp_outer, rows, q_width)
        g_out = ring_reduce(g_out, inv_batch, 1, "z", "x", 5)

        gqkv = attn_bwd(qkv, grad_attn, lse, cos_all, sin_all, attn_blk)
        gqkv_tok = to_heads(gqkv.reshape(sp_size, n_local, q_width + 2 * k_width))
        flat = lambda t: jnp.transpose(t, (1, 0, 2)).reshape(n_local, -1)
        grad_normed = (
            nt(flat(gqkv_tok[:, :, :q_width]), w_query)
            + nt(flat(gqkv_tok[:, :, q_width : q_width + k_width]), w_key)
            + nt(flat(gqkv_tok[:, :, q_width + k_width :]), w_value)
        ).astype(BF16)
        grad_tok_norm, g_norm_attn = norm_bwd(grad_normed, unit_attn, inv_attn, norm_attn)
        grad_tokens = (grad_hidden.astype(F32) + grad_tok_norm).astype(BF16)

        g_attn = tn(normed_full, gqkv).astype(BF16).reshape(dp_size, rows, q_width + 2 * k_width)
        gains = jnp.stack([g_norm_attn.reshape(dp_size, rows), g_norm_mlp.reshape(dp_size, rows)], axis=1)
        gains = jnp.pad(gains.astype(BF16), ((0, 0), (0, rows - 2), (0, 0)))
        g_attn = ring_reduce(jnp.concatenate([g_attn, gains], axis=2), inv_batch, 2, "z", "y", 2)
        g_attn = gather(jnp.concatenate([g_attn, g_out], axis=1), ("z", "y", "x", "c"))

        g_gate, g_up, g_down = spread_mlp(g_mlp, mlp_outer, mlp_size, ff_local)
        g_query, g_key, g_value, g_out, gains = spread_attn(g_attn, side, dp_size // side, sp_size, q_width, k_width)
        gains = gains.reshape(dp_size, 8, rows)
        return (
            grad_tokens[None],
            gains[:, 0].reshape(dim),
            g_query,
            g_key,
            g_value,
            g_out,
            gains[:, 1].reshape(dim),
            g_gate,
            g_up,
            g_down,
        )

    return jax.shard_map(device_step, mesh=grid, in_specs=(seq_spec, seq_spec) + (P(),) * 9, out_specs=(seq_spec,) + (P(),) * 9, check_vma=False)
```

```python
import functools
import math

import jax
import jax.numpy as jnp
from jax import lax
from jax.experimental import pallas as pl
from jax.experimental.pallas import tpu as pltpu
from jax.sharding import PartitionSpec as P


NORM_EPS = 1.0e-5
ROPE_BASE = 1.0e6
HEAD_DIM = 128
F32 = jnp.float32
BF16 = jnp.bfloat16
VMEM_LIMIT = 60 * 1024 * 1024
MESH = pl.DeviceIdType.MESH
NEG = -1.0e30


def nn(a, b):
    return lax.dot_general(a, b, (((1,), (0,)), ((), ())), preferred_element_type=F32)


def nt(a, b):
    return lax.dot_general(a, b, (((1,), (1,)), ((), ())), preferred_element_type=F32)


def tn(a, b):
    return lax.dot_general(a, b, (((0,), (0,)), ((), ())), preferred_element_type=F32)


def norm_fwd(values, gain_vec):
    values_f = values.astype(F32)
    inv_rms = lax.rsqrt(jnp.mean(values_f * values_f, axis=-1, keepdims=True) + NORM_EPS)
    unit_vals = values_f * inv_rms
    return (unit_vals * gain_vec.astype(F32)).astype(BF16), unit_vals, inv_rms


def norm_bwd(grad_normed, unit_vals, inv_rms, gain_vec):
    grad_f = grad_normed.astype(F32)
    grad_gain = jnp.sum(grad_f * unit_vals, axis=0)
    grad_unit = grad_f * gain_vec.astype(F32)
    grad_in = inv_rms * (grad_unit - unit_vals * jnp.mean(grad_unit * unit_vals, axis=-1, keepdims=True))
    return grad_in, grad_gain


def rope_tables(positions):
    half_dim = HEAD_DIM // 2
    inv_freq = ROPE_BASE ** (-jnp.arange(half_dim, dtype=F32) * (2.0 / HEAD_DIM))
    angles = positions.astype(F32)[:, None] * inv_freq[None, :]
    cos, sin = jnp.cos(angles), jnp.sin(angles)
    return jnp.concatenate([cos, cos], axis=-1), jnp.concatenate([-sin, sin], axis=-1)


def rope(values, cos_tab, sin_tab):
    return values * cos_tab + pltpu.roll(values, HEAD_DIM // 2, 1) * sin_tab


def call(kernel, flops, moved, **kwargs):
    params = pltpu.CompilerParams(vmem_limit_bytes=VMEM_LIMIT)
    cost = pl.CostEstimate(flops=int(flops), bytes_accessed=int(moved), transcendentals=0)
    return pl.pallas_call(kernel, compiler_params=params, cost_estimate=cost, **kwargs)


def whole(shape):
    return pl.BlockSpec(shape, lambda *_: (0,) * len(shape))


def gather_qkv_kernel(x_ref, wq_ref, wk_ref, wv_ref, cos_blk, sin_blk, cos_row, sin_row, full_ref, qkv_ref, land, weights, w_sems, o_sems, i_send, i_recv, d_send, d_recv):
    x, c = lax.axis_index("x"), lax.axis_index("c")
    n = land.shape[0] // 2
    tok = x_ref.shape[0]
    half = tok // 2
    qw, kw = wq_ref.shape[1] // (2 * n), wk_ref.shape[1] // (2 * n)
    width = qw + 2 * kw
    wrap = lambda v: lax.rem(v + 2 * n, n)
    at = lambda dx, core: 2 * wrap(x + dx) + core
    me = 2 * x + c

    loads = []
    for k, (ref, start, size) in enumerate(((wq_ref, 0, qw), (wk_ref, qw, kw), (wv_ref, qw + kw, kw))):
        cols = pl.ds(pl.multiple_of(me * size, 128), size)
        loads.append(pltpu.make_async_copy(ref.at[:, cols], weights.at[:, pl.ds(start, size)], w_sems.at[k]))
        loads[-1].start()

    barrier = pltpu.get_barrier_semaphore()
    for goal in ({"x": wrap(x + 1)}, {"x": wrap(x - 1)}, {"c": 1 - c}):
        pl.semaphore_signal(barrier, inc=1, device_id=goal, device_id_type=MESH)
    pl.semaphore_wait(barrier, 3)

    rows = lambda h: pl.ds(h * half, half)

    def ring(way, hop, h):
        k = (0 if way > 0 else 3) + (h if hop == 0 else 2)
        src = land.at[at(-way * hop, c), rows(h)] if hop else x_ref.at[rows(h)]
        dst = land.at[at(-way * hop, c), rows(h)]
        return pltpu.make_async_remote_copy(src, dst, i_send.at[k], i_recv.at[k], device_id={"x": wrap(x + way)}, device_id_type=MESH)

    def across(k, dx, h):
        part = rows(h) if h is not None else pl.ds(0, tok)
        src = land.at[at(dx, c), part] if dx else x_ref.at[part]
        return pltpu.make_async_remote_copy(src, land.at[at(dx, c), part], d_send.at[k], d_recv.at[k], device_id={"c": 1 - c}, device_id_type=MESH)

    first = [ring(1, 0, 0), ring(-1, 0, 1), ring(1, 0, 1), ring(-1, 0, 0)]
    second = [ring(1, 1, 0), ring(-1, 1, 1)]
    die = [across(0, 0, None), across(1, -1, 0), across(2, 1, 1), across(3, -1, 1), across(4, 1, 0), across(5, 2, 0), across(6, 2, 1)]
    for copy in first[:2] + die[:1] + first[2:]:
        copy.start()
    land[me] = x_ref[...]
    for load in loads:
        load.wait()

    def wait_block(k):
        @pl.when(k == 1)
        def _():
            die[0].wait_recv()

        @pl.when(k == 2)
        def _():
            first[0].wait_recv()
            second[0].start()
            die[1].start()
            first[1].wait_recv()
            second[1].start()
            die[2].start()
            first[2].wait_recv()
            die[3].start()

        @pl.when(k == 3)
        def _():
            first[3].wait_recv()
            die[4].start()

        @pl.when(k == 4)
        def _():
            die[1].wait_recv()
            die[3].wait_recv()

        @pl.when(k == 5)
        def _():
            die[2].wait_recv()
            die[4].wait_recv()

        @pl.when(k == 6)
        def _():
            second[0].wait_recv()
            die[5].start()
            second[1].wait_recv()
            die[6].start()

        @pl.when(k == 7)
        def _():
            die[5].wait_recv()
            die[6].wait_recv()

    def out_copy(k):
        dx = jnp.where(k < 2, 0, jnp.where(k >= 6, 2, jnp.where(lax.rem(k, 2) == 0, -1, 1)))
        core = jnp.where((k == 1) | (k == 4) | (k == 5) | (k == 7), 1 - c, c)
        block = 2 * wrap(x + dx) + core
        here = pl.ds(pl.multiple_of(block * tok, tok), tok)
        return block, here, pltpu.make_async_copy(land.at[block], full_ref.at[here, :], o_sems.at[k])

    def body(k, carry):
        wait_block(k)
        block, here, copy = out_copy(k)
        copy.start()
        value = nn(land[block], weights[...])
        cos_b, sin_b = cos_blk[pl.ds(block, 1), :], sin_blk[pl.ds(block, 1), :]
        cos = cos_b * cos_row[...] - sin_b * sin_row[...]
        sin = sin_b * cos_row[...] + cos_b * sin_row[...]
        for start in range(0, width, HEAD_DIM):
            part = value[:, start : start + HEAD_DIM]
            if start < qw + kw:
                part = rope(part, cos, sin)
            qkv_ref[here, start : start + HEAD_DIM] = part.astype(BF16)
        return carry

    lax.fori_loop(0, 2 * n, body, 0)
    for copy in first + second + die:
        copy.wait_send()
    for k in range(2 * n):
        out_copy(k)[2].wait()


def gather_qkv(normed, w_query, w_key, w_value, groups, collective_id):
    tok, dim = normed.shape
    width = (w_query.shape[1] + w_key.shape[1] + w_value.shape[1]) // groups
    anywhere = pl.BlockSpec(memory_space=pl.ANY)
    vmem = pl.BlockSpec(memory_space=pltpu.VMEM)
    return pl.pallas_call(
        gather_qkv_kernel,
        in_specs=[vmem, anywhere, anywhere, anywhere, vmem, vmem, vmem, vmem],
        out_specs=[anywhere, vmem],
        out_shape=[jax.ShapeDtypeStruct((groups * tok, dim), BF16), jax.ShapeDtypeStruct((groups * tok, width), BF16)],
        scratch_shapes=[
            pltpu.VMEM((groups, tok, dim), BF16),
            pltpu.VMEM((dim, width), BF16),
            pltpu.SemaphoreType.DMA((3,)),
            pltpu.SemaphoreType.DMA((groups,)),
            pltpu.SemaphoreType.DMA((6,)),
            pltpu.SemaphoreType.DMA((6,)),
            pltpu.SemaphoreType.DMA((7,)),
            pltpu.SemaphoreType.DMA((7,)),
        ],
        compiler_params=pltpu.CompilerParams(collective_id=collective_id, has_side_effects=True, vmem_limit_bytes=VMEM_LIMIT),
        cost_estimate=pl.CostEstimate(flops=20_000_000_000, bytes_accessed=6 * groups * tok * dim, transcendentals=0),
        name="gather_qkv",
    )(normed, w_query, w_key, w_value, *rope_tables(jnp.arange(groups) * tok), *rope_tables(jnp.arange(tok)))


def attn_fwd_kernel(blk, n_q, qkv_ref, out_ref, lse_ref, tok_ref, mine, land, send_sems, recv_sems, *scrs):
    step, steps = pl.program_id(0), pl.num_programs(0)
    x, c = lax.axis_index("x"), lax.axis_index("c")
    me = 2 * x + c
    tok = blk // 2

    def block_of(step):
        ahead = jnp.where(step == 0, 2, jnp.where(step == 1, 1, jnp.where(step == 2, steps - 1, 0)))
        return lax.rem(x + ahead, steps)

    def send(step, core):
        goal = block_of(step)
        src = mine.at[2 * goal + core]
        return pltpu.make_async_remote_copy(src, land.at[me], send_sems.at[step, core], recv_sems.at[me], device_id={"x": goal, "c": core}, device_id_type=MESH)

    @pl.when(step == 0)
    def _():
        barrier = pltpu.get_barrier_semaphore()
        for k in range(1, 2 * steps):
            peer = lax.rem(me + k, 2 * steps)
            pl.semaphore_signal(barrier, inc=1, device_id={"x": peer // 2, "c": lax.rem(peer, 2)}, device_id_type=MESH)
        pl.semaphore_wait(barrier, 2 * steps - 1)

    @pl.when(step > 0)
    def _():
        send(step - 1, 0).start()
        send(step - 1, 1).start()

    i = block_of(step)
    coef = HEAD_DIM**-0.5 * math.log2(math.e)
    k_at, v_at = n_q * HEAD_DIM, (n_q + 1) * HEAD_DIM
    at = lambda j: pl.ds(pl.multiple_of(j * blk, blk), blk)
    lanes = lambda t, op: functools.reduce(op, [t[:, s : s + 128] for s in range(0, blk, 128)])
    qs = [qkv_ref[at(i), h * HEAD_DIM : (h + 1) * HEAD_DIM] for h in range(n_q)]
    causal = lax.broadcasted_iota(jnp.int32, (blk, blk), 0) >= lax.broadcasted_iota(jnp.int32, (blk, blk), 1)

    def score_step(j, tops, masked):
        key = qkv_ref[at(j), k_at:v_at]
        new = []
        for h in range(n_q):
            s = nt(qs[h], key)
            if masked:
                s = jnp.where(causal, s, NEG)
            scrs[h][:, at(j)] = s
            new.append(jnp.maximum(tops[h], lanes(s, jnp.maximum)))
        return tuple(new)

    start = tuple(jnp.full((blk, 128), NEG, F32) for _ in range(n_q))
    tops = lax.fori_loop(0, i, lambda j, t: score_step(j, t, False), start)
    tops = score_step(i, tops, True)
    row_max = [jnp.max(t, axis=1, keepdims=True) for t in tops]

    def exp_step(j, sums):
        new = []
        for h in range(n_q):
            e = jnp.exp2((scrs[h][:, at(j)] - row_max[h]) * coef)
            scrs[h][:, at(j)] = e
            new.append(sums[h] + lanes(e, jnp.add))
        return tuple(new)

    sums = lax.fori_loop(0, i + 1, exp_step, tuple(jnp.zeros((blk, 128), F32) for _ in range(n_q)))
    row_sum = [jnp.sum(t, axis=1, keepdims=True) for t in sums]
    inv_sum = [1.0 / t for t in row_sum]

    def out_step(j, accs):
        value = qkv_ref[at(j), v_at : v_at + HEAD_DIM]
        return tuple(accs[h] + nn((scrs[h][:, at(j)] * inv_sum[h]).astype(BF16), value) for h in range(n_q))

    accs = lax.fori_loop(0, i + 1, out_step, tuple(jnp.zeros((blk, HEAD_DIM), F32) for _ in range(n_q)))
    for h in range(n_q):
        value = accs[h].astype(BF16)
        out_ref[at(i), h * HEAD_DIM : (h + 1) * HEAD_DIM] = value
        for core in range(2):
            mine[2 * i + core, :, h * HEAD_DIM : (h + 1) * HEAD_DIM] = value[core * tok : (core + 1) * tok, :]
        log_norm = row_max[h] * coef + jnp.log2(row_sum[h])
        lse_ref[h * 8 : (h + 1) * 8, at(i)] = jnp.transpose(jnp.broadcast_to(log_norm, (blk, 128)))[:8, :]

    @pl.when(step == steps - 1)
    def _():
        land[me] = mine[me]
        send(step, 1 - c).start()
        for k in range(1, 2 * steps):
            peer = lax.rem(me + k, 2 * steps)
            pltpu.make_async_remote_copy(mine.at[peer], land.at[peer], send_sems.at[0, 0], recv_sems.at[peer], device_id={"x": x, "c": c}, device_id_type=MESH).wait_recv()
        tok_ref[...] = land[...]
        for k in range(steps - 1):
            send(k, 0).wait_send()
            send(k, 1).wait_send()
        send(step, 1 - c).wait_send()


def attn_fwd(qkv, steps, collective_id):
    seq, width = qkv.shape
    n_q = width // HEAD_DIM - 2
    blk = seq // steps
    return pl.pallas_call(
        functools.partial(attn_fwd_kernel, blk, n_q),
        grid=(steps,),
        in_specs=[whole((seq, width))],
        out_specs=[whole((seq, n_q * HEAD_DIM)), whole((8 * n_q, seq)), whole((2 * steps, blk // 2, n_q * HEAD_DIM))],
        out_shape=[
            jax.ShapeDtypeStruct((seq, n_q * HEAD_DIM), BF16),
            jax.ShapeDtypeStruct((8 * n_q, seq), F32),
            jax.ShapeDtypeStruct((2 * steps, blk // 2, n_q * HEAD_DIM), BF16),
        ],
        scratch_shapes=[pltpu.VMEM((2 * steps, blk // 2, n_q * HEAD_DIM), BF16)] * 2
        + [pltpu.SemaphoreType.DMA((steps, 2)), pltpu.SemaphoreType.DMA((2 * steps,))]
        + [pltpu.VMEM((blk, seq), F32)] * n_q,
        compiler_params=pltpu.CompilerParams(collective_id=collective_id, has_side_effects=True, vmem_limit_bytes=VMEM_LIMIT),
        cost_estimate=pl.CostEstimate(flops=2 * n_q * seq * seq * HEAD_DIM * 2, bytes_accessed=seq * width * 2, transcendentals=0),
        name="attn_fwd",
    )(qkv)


def attn_bwd_kernel(blk, n_q, qkv_ref, do_ref, lse_ref, cos_ref, sin_ref, out_ref, dk_scr, dv_scr, *scrs):
    i, steps = pl.program_id(0), pl.num_programs(0)
    scale = HEAD_DIM**-0.5
    coef = scale * math.log2(math.e)
    k_at, v_at = n_q * HEAD_DIM, (n_q + 1) * HEAD_DIM
    at = lambda j: pl.ds(pl.multiple_of(j * blk, blk), blk)
    p_scrs, dp_scrs = scrs[:n_q], scrs[n_q:]
    qs = [qkv_ref[at(i), h * HEAD_DIM : (h + 1) * HEAD_DIM] for h in range(n_q)]
    dos = [do_ref[:, h * HEAD_DIM : (h + 1) * HEAD_DIM] for h in range(n_q)]
    lses = [lse_ref[h * 8 : h * 8 + 1, :] for h in range(n_q)]
    causal = lax.broadcasted_iota(jnp.int32, (blk, blk), 0) <= lax.broadcasted_iota(jnp.int32, (blk, blk), 1)

    @pl.when(i == 0)
    def _():
        dk_scr[...] = jnp.zeros_like(dk_scr)
        dv_scr[...] = jnp.zeros_like(dv_scr)

    def prob_step(j, dots, masked):
        key, value = qkv_ref[at(j), k_at:v_at], qkv_ref[at(j), v_at : v_at + HEAD_DIM]
        new, dv = [], dv_scr[at(j), :]
        for h in range(n_q):
            p = jnp.exp2(nt(key, qs[h]) * coef - lses[h])
            if masked:
                p = jnp.where(causal, p, 0.0)
            dp = nt(value, dos[h]).astype(BF16)
            p_scrs[h][at(j), :] = p
            dp_scrs[h][at(j), :] = dp
            dv = dv + nn(p.astype(BF16), dos[h])
            new.append(dots[h] + jnp.sum((p * dp.astype(F32)).reshape(blk // 8, 8, blk), axis=0))
        dv_scr[at(j), :] = dv
        return tuple(new)

    dots = lax.fori_loop(0, i, lambda j, t: prob_step(j, t, False), tuple(jnp.zeros((8, blk), F32) for _ in range(n_q)))
    dots = prob_step(i, dots, True)
    row_dot = [jnp.sum(t, axis=0, keepdims=True) for t in dots]

    def grad_step(j, accs):
        key = qkv_ref[at(j), k_at:v_at]
        new, dk = [], dk_scr[at(j), :]
        for h in range(n_q):
            ds = (p_scrs[h][at(j), :] * (dp_scrs[h][at(j), :].astype(F32) - row_dot[h]) * scale).astype(BF16)
            dk = dk + nn(ds, qs[h])
            new.append(accs[h] + tn(ds, key))
        dk_scr[at(j), :] = dk
        return tuple(new)

    accs = lax.fori_loop(0, i + 1, grad_step, tuple(jnp.zeros((blk, HEAD_DIM), F32) for _ in range(n_q)))
    unrope = lambda g, sl: rope(g.astype(BF16).astype(F32), cos_ref[sl, :], -sin_ref[sl, :]).astype(BF16)
    for h in range(n_q):
        out_ref[at(i), h * HEAD_DIM : (h + 1) * HEAD_DIM] = unrope(accs[h], at(i))

    @pl.when(i == steps - 1)
    def _():
        def finish(j, carry):
            out_ref[at(j), k_at:v_at] = unrope(dk_scr[at(j), :], at(j))
            out_ref[at(j), v_at : v_at + HEAD_DIM] = dv_scr[at(j), :].astype(BF16)
            return carry

        lax.fori_loop(0, steps, finish, 0)


def attn_bwd(qkv, grad_out, lse, cos, sin, blk):
    seq, width = qkv.shape
    n_q = width // HEAD_DIM - 2
    return call(
        functools.partial(attn_bwd_kernel, blk, n_q),
        5 * n_q * seq * seq * HEAD_DIM * 2,
        seq * width * 4,
        grid=(seq // blk,),
        in_specs=[
            whole((seq, width)),
            pl.BlockSpec((blk, n_q * HEAD_DIM), lambda i: (i, 0)),
            pl.BlockSpec((8 * n_q, blk), lambda i: (0, i)),
            whole((seq, HEAD_DIM)),
            whole((seq, HEAD_DIM)),
        ],
        out_specs=whole((seq, width)),
        out_shape=jax.ShapeDtypeStruct((seq, width), BF16),
        scratch_shapes=[pltpu.VMEM((seq, HEAD_DIM), F32)] * 2
        + [pltpu.VMEM((seq, blk), F32)] * n_q
        + [pltpu.VMEM((seq, blk), BF16)] * n_q,
        name="attn_bwd",
    )(qkv, grad_out, lse, cos, sin)


def act_grads(gate, up, grad_act):
    sig = 1.0 / (1.0 + jnp.exp(-gate))
    act = gate * sig
    grad_gate = (grad_act * up * sig * (1.0 + gate * (1.0 - sig))).astype(BF16)
    grad_up = (grad_act * act).astype(BF16)
    return (act * up).astype(BF16), grad_gate, grad_up


def mlp_kernel(m_ref, dy_ref, wg_ref, wu_ref, wd_ref, out_ref, acc_ref):
    step = pl.program_id(0)
    m, dy = m_ref[...], dy_ref[...]
    grad_act = nt(dy, wd_ref[...]).astype(BF16).astype(F32)
    _, grad_gate, grad_up = act_grads(nn(m, wg_ref[...]), nn(m, wu_ref[...]), grad_act)
    total = nt(grad_gate, wg_ref[...]) + nt(grad_up, wu_ref[...])

    @pl.when(step == 0)
    def _():
        acc_ref[...] = total

    @pl.when(step > 0)
    def _():
        acc_ref[...] += total

    @pl.when(step == pl.num_programs(0) - 1)
    def _():
        out_ref[...] = acc_ref[...].astype(BF16)


def mlp_grad_input(m, dy, w_gate, w_up, w_down, blk):
    tok, dim = m.shape
    width = w_gate.shape[1]
    return call(
        mlp_kernel,
        5 * 2 * tok * dim * width,
        3 * 2 * dim * width,
        grid=(width // blk,),
        in_specs=[
            whole((tok, dim)),
            whole((tok, dim)),
            pl.BlockSpec((dim, blk), lambda j: (0, j)),
            pl.BlockSpec((dim, blk), lambda j: (0, j)),
            pl.BlockSpec((blk, dim), lambda j: (j, 0)),
        ],
        out_specs=whole((tok, dim)),
        out_shape=jax.ShapeDtypeStruct((tok, dim), BF16),
        scratch_shapes=[pltpu.VMEM((tok, dim), F32)],
        name="mlp_grad_input",
    )(m, dy, w_gate, w_up, w_down)


class Ring:
    def __init__(self, n, subs, slow, fast, source, recv1, acc, send2, recv2, s1, r1, s2, r2):
        self.n, self.subs, self.slow, self.fast, self.source = n, subs, slow, fast, source
        self.recv1, self.acc, self.send2, self.recv2 = recv1, acc, send2, recv2
        self.s1, self.r1, self.s2, self.r2 = s1, r1, s2, r2
        self.z, self.y = lax.axis_index(slow), lax.axis_index(fast)
        self.height = recv1.shape[5]

    def wrap(self, v):
        return lax.rem(v + 2 * self.n, self.n)

    def goal(self, c, phase):
        step = 1 - 2 * (c % 2)
        if (c < 2) == (phase == 1):
            return {self.fast: self.wrap(self.y + step)}
        return {self.slow: self.wrap(self.z + step)}

    def arrive(self):
        barrier = pltpu.get_barrier_semaphore()
        for c in range(4):
            pl.semaphore_signal(barrier, inc=1, device_id=self.goal(c, 1), device_id_type=MESH)

    def meet(self):
        pl.semaphore_wait(pltpu.get_barrier_semaphore(), 4)

    def coord(self, c, phase):
        return self.y if (c < 2) == (phase == 1) else self.z

    def rows(self, c, s):
        return pl.ds((c * self.subs + s) * self.height, self.height)

    def local(self, b, c, a, s):
        source = self.source(b)
        return source.at[:, a, self.rows(c, s), :] if c < 2 else source.at[a, :, self.rows(c, s), :]

    def chunk(self, c, phase, t):
        return self.wrap(self.coord(c, phase) - (1 - 2 * (c % 2)) * t)

    def copy1(self, b, c, t, s):
        src = self.recv1.at[b, c, t - 1, s] if t else self.local(b, c, self.chunk(c, 1, 1), s)
        dst = self.recv1.at[b, c, t, s]
        return pltpu.make_async_remote_copy(src, dst, self.s1.at[b, c, t, s], self.r1.at[b, c, t, s], device_id=self.goal(c, 1), device_id_type=MESH)

    def copy2(self, b, c, t, s):
        src = self.recv2.at[b, c, t - 1, s] if t else self.send2.at[b, c, s]
        dst = self.recv2.at[b, c, t, s]
        return pltpu.make_async_remote_copy(src, dst, self.s2.at[b, c, t, s], self.r2.at[b, c, t, s], device_id=self.goal(c, 2), device_id_type=MESH)

    def start(self, b):
        for s in range(self.subs):
            for c in range(4):
                self.copy1(b, c, 0, s).start()

    def hop1(self, b, t):
        for s in range(self.subs):
            for c in range(4):
                self.copy1(b, c, t, s).wait_recv()
                mine = self.local(b, c, self.chunk(c, 1, t + 2), s)[...]
                total = self.recv1[b, c, t, s].astype(F32) + mine.astype(F32)
                if t < self.n - 2:
                    self.recv1[b, c, t, s] = total.astype(BF16)
                    self.copy1(b, c, t + 1, s).start()
                else:
                    self.acc[b, c, s] = total
                    self.send2[b, c, s] = self.acc[b, c, s, self.chunk(c, 2, 1)].astype(BF16)
                    self.copy2(b, c, 0, s).start()

    def hop2(self, b, t, scale, store):
        for s in range(self.subs):
            for c in range(4):
                self.copy2(b, c, t, s).wait_recv()
                total = self.recv2[b, c, t, s].astype(F32) + self.acc[b, c, s, self.chunk(c, 2, t + 2)]
                if t < self.n - 2:
                    self.recv2[b, c, t, s] = total.astype(BF16)
                    self.copy2(b, c, t + 1, s).start()
                else:
                    store(b, (c * self.subs + s) * self.height, self.height, (total * scale).astype(BF16))

    def drain(self, b):
        for s in range(self.subs):
            for c in range(4):
                for t in range(self.n - 1):
                    self.copy1(b, c, t, s).wait_send()
                    self.copy2(b, c, t, s).wait_send()

    @staticmethod
    def scratch(n, blocks, subs, rows, width):
        height = rows // (4 * subs)
        return [
            pltpu.VMEM((blocks, 4, n - 1, subs, n, height, width), BF16),
            pltpu.VMEM((blocks, 4, subs, n, height, width), F32),
            pltpu.VMEM((blocks, 4, subs, height, width), BF16),
            pltpu.VMEM((blocks, 4, n - 1, subs, height, width), BF16),
        ] + [pltpu.SemaphoreType.DMA((blocks, 4, n - 1, subs))] * 4


def mlp_ring_kernel(n, subs, scale, blocks, slow, fast, group, m_all, dy_all, wg_all, wu_all, wd_all, out_ref, m_ref, dy_ref, in_sems, wg_buf, wu_buf, wd_buf, w_sems, grads_ref, act_ref, g_ref, *scratch):
    step = pl.program_id(0)
    seq, dim = m_ref.shape
    width = act_ref.shape[0]
    rows = dim // (n * n)
    tiles = 4
    blk, tile = seq // tiles, dim // tiles
    per_tile = tile // rows
    ring = Ring(n, subs, slow, fast, lambda b: g_ref.at[b], *scratch)
    at = lambda i, size: pl.ds(pl.multiple_of(i * size, size), size)

    def loads(b):
        mine = at((lax.axis_index(group) if group else 0) * blocks + b, width)
        slot = lax.rem(b, 2)
        return [
            pltpu.make_async_copy(wg_all.at[:, mine], wg_buf.at[slot], w_sems.at[slot, 0]),
            pltpu.make_async_copy(wu_all.at[:, mine], wu_buf.at[slot], w_sems.at[slot, 1]),
            pltpu.make_async_copy(wd_all.at[mine, :], wd_buf.at[slot], w_sems.at[slot, 2]),
        ]

    def tokens(i):
        return [
            pltpu.make_async_copy(m_all.at[at(i, blk), :], m_ref.at[at(i, blk), :], in_sems.at[0, i]),
            pltpu.make_async_copy(dy_all.at[at(i, blk), :], dy_ref.at[at(i, blk), :], in_sems.at[1, i]),
        ]

    @pl.when(step == 0)
    def _():
        for load in loads(0) + [load for i in range(tiles) for load in tokens(i)]:
            load.start()
        ring.arrive()
        ring.meet()

    @pl.when(step + 1 < blocks)
    def _():
        for load in loads(step + 1):
            load.start()

    for load in loads(step):
        load.wait()
    wg_ref, wu_ref, wd_ref = (buf.at[lax.rem(step, 2)] for buf in (wg_buf, wu_buf, wd_buf))

    def store(b, first, height, value):
        out_ref[pl.ds(pl.multiple_of(b * 3 * width + first, height), height), :] = value

    hops = [functools.partial(ring.hop1, t=t) for t in range(n - 1)]
    hops += [functools.partial(ring.hop2, t=t, scale=scale, store=store) for t in range(n - 1)]
    slots = 2 * tiles
    delays = [3 * t + 3 if t < n - 1 else 3 * n - 1 + 2 * (t - n + 1) for t in range(2 * (n - 1))]

    def events(slot):
        for hop, delay in zip(hops, delays):
            since = slot - delay
            block = since // slots - 1

            @pl.when((since >= slots) & (lax.rem(since, slots) == 0) & (block < blocks))
            def _(hop=hop, block=block):
                hop(block)

    def forward(i):
        @pl.when(step == 0)
        def _():
            for load in tokens(i):
                load.wait()

        m, dy = m_ref[at(i, blk), :], dy_ref[at(i, blk), :]
        grad_act = nt(dy, wd_ref[...]).astype(BF16).astype(F32)
        act, grad_gate, grad_up = act_grads(nn(m, wg_ref[...]), nn(m, wu_ref[...]), grad_act)
        act_ref[:, at(i, blk)] = jnp.transpose(act)
        grads_ref[:width, at(i, blk)] = jnp.transpose(grad_gate)
        grads_ref[width:, at(i, blk)] = jnp.transpose(grad_up)

    def weights(i):
        grads = nn(grads_ref[...], m_ref[:, at(i, tile)]).astype(BF16)
        down = nn(act_ref[...], dy_ref[:, at(i, tile)]).astype(BF16)
        for k in range(per_tile):
            piece = i * per_tile + k
            g_ref[step, piece // n, lax.rem(piece, n), : 2 * width, :] = grads[:, k * rows : (k + 1) * rows]
            g_ref[step, piece // n, lax.rem(piece, n), 2 * width :, :] = down[:, k * rows : (k + 1) * rows]

    def slot_body(i, carry):
        @pl.when(i < tiles)
        def _():
            forward(i)

        @pl.when(i >= tiles)
        def _():
            weights(i - tiles)

        events(step * slots + i)
        return carry

    lax.fori_loop(0, slots, slot_body, 0)
    ring.start(step)

    @pl.when(step == blocks - 1)
    def _():
        def tail(slot, carry):
            events(slot)
            return carry

        lax.fori_loop(blocks * slots, (blocks + 1) * slots + max(delays), tail, 0)

        def drain(b, carry):
            ring.drain(b)
            return carry

        lax.fori_loop(0, blocks, drain, 0)


def mlp_ring(m, dy, w_gate, w_up, w_down, ff, scale, slow, fast, n, group, collective_id):
    seq, dim = m.shape
    width = min(256, ff)
    blocks = ff // width
    subs = 2
    rows = dim // (n * n)
    anywhere = pl.BlockSpec(memory_space=pl.ANY)
    return pl.pallas_call(
        functools.partial(mlp_ring_kernel, n, subs, scale, blocks, slow, fast, group),
        grid=(blocks,),
        in_specs=[anywhere] * 5,
        out_specs=pl.BlockSpec((3 * ff, rows), lambda j: (0, 0)),
        scratch_shapes=[
            pltpu.VMEM((seq, dim), BF16),
            pltpu.VMEM((seq, dim), BF16),
            pltpu.SemaphoreType.DMA((2, 4)),
            pltpu.VMEM((2, dim, width), BF16),
            pltpu.VMEM((2, dim, width), BF16),
            pltpu.VMEM((2, width, dim), BF16),
            pltpu.SemaphoreType.DMA((2, 3)),
            pltpu.VMEM((2 * width, seq), BF16),
            pltpu.VMEM((width, seq), BF16),
            pltpu.VMEM((blocks, n, n, 3 * width, rows), BF16),
        ]
        + Ring.scratch(n, blocks, subs, 3 * width, rows),
        out_shape=jax.ShapeDtypeStruct((3 * ff, rows), BF16),
        compiler_params=pltpu.CompilerParams(collective_id=collective_id, has_side_effects=True, vmem_limit_bytes=VMEM_LIMIT),
        cost_estimate=pl.CostEstimate(flops=18 * seq * dim * ff, bytes_accessed=4 * seq * dim, transcendentals=0),
        name="mlp_ring",
    )(m, dy, w_gate, w_up, w_down)


def ring_reduce_kernel(n, subs, scale, slow, fast, g_ref, out_ref, *scratch):
    ring = Ring(n, subs, slow, fast, lambda b: g_ref, *scratch)

    def store(b, first, height, value):
        out_ref[first : first + height, :] = value

    ring.arrive()
    ring.meet()
    ring.start(0)
    for t in range(n - 1):
        ring.hop1(0, t)
    for t in range(n - 1):
        ring.hop2(0, t, scale, store)
    ring.drain(0)


def ring_reduce(pieces, scale, subs, slow, fast, collective_id):
    total, rows, width = pieces.shape
    n = round(total**0.5)
    return pl.pallas_call(
        functools.partial(ring_reduce_kernel, n, subs, scale, slow, fast),
        out_shape=jax.ShapeDtypeStruct((rows, width), BF16),
        in_specs=[pl.BlockSpec(memory_space=pltpu.VMEM)],
        out_specs=pl.BlockSpec(memory_space=pltpu.VMEM),
        scratch_shapes=Ring.scratch(n, 1, subs, rows, width),
        compiler_params=pltpu.CompilerParams(collective_id=collective_id, has_side_effects=True, vmem_limit_bytes=VMEM_LIMIT),
        cost_estimate=pl.CostEstimate(flops=40_000_000_000, bytes_accessed=2 * total * rows * width, transcendentals=0),
        name="ring_reduce",
    )(pieces.reshape(n, n, rows, width))


def spread_mlp_kernel(groups, ff_local, width, in_ref, gate_ref, up_ref, down_ref):
    for g in range(groups):
        for at in range(g * ff_local, (g + 1) * ff_local, width):
            gate_ref[:, at : at + width] = jnp.transpose(in_ref[3 * at : 3 * at + width, :]).astype(F32)
            up_ref[:, at : at + width] = jnp.transpose(in_ref[3 * at + width : 3 * at + 2 * width, :]).astype(F32)
            down_ref[at : at + width, :] = in_ref[3 * at + 2 * width : 3 * at + 3 * width, :].astype(F32)


def spread_mlp(stacked, outer, groups, ff_local):
    total, rows = stacked.shape
    ff, dim = ff_local * groups, rows * outer
    return call(
        functools.partial(spread_mlp_kernel, groups, ff_local, min(256, ff_local)),
        total * rows,
        total * rows * 6,
        grid=(outer,),
        in_specs=[pl.BlockSpec((total // outer, rows), lambda o: (o, 0))],
        out_specs=[
            pl.BlockSpec((rows, ff), lambda o: (o, 0)),
            pl.BlockSpec((rows, ff), lambda o: (o, 0)),
            pl.BlockSpec((ff, rows), lambda o: (0, o)),
        ],
        out_shape=[jax.ShapeDtypeStruct((dim, ff), F32)] * 2 + [jax.ShapeDtypeStruct((ff, dim), F32)],
        name="spread_mlp",
    )(stacked)


def spread_attn_kernel(groups, q_width, k_width, in_ref, q_ref, k_ref, v_ref, o_ref, gain_ref):
    rows = q_ref.shape[0]
    gain = None
    for g in range(groups):
        first = g * (rows + 8)
        piece = in_ref[first : first + rows, :].astype(F32)
        q_ref[:, g * q_width : (g + 1) * q_width] = piece[:, :q_width]
        k_ref[:, g * k_width : (g + 1) * k_width] = piece[:, q_width : q_width + k_width]
        v_ref[:, g * k_width : (g + 1) * k_width] = piece[:, q_width + k_width : q_width + 2 * k_width]
        block, core = g // 2, g % 2
        o_ref[core * q_width : (core + 1) * q_width, block * rows : (block + 1) * rows] = jnp.transpose(piece[:, q_width + 2 * k_width :])
        part = in_ref[first + rows : first + rows + 8, :rows].astype(F32)
        gain = part if gain is None else gain + part
    gain_ref[...] = gain


def spread_attn(stacked, nz, ny, groups, q_width, k_width):
    total, row_width = stacked.shape
    outer = nz * ny
    rows = total // (outer * groups) - 8
    dim = rows * outer
    nx = groups // 2
    return call(
        functools.partial(spread_attn_kernel, groups, q_width, k_width),
        total * row_width,
        total * row_width * 6,
        grid=(outer,),
        in_specs=[pl.BlockSpec((total // outer, row_width), lambda o: (o, 0))],
        out_specs=[
            pl.BlockSpec((rows, groups * q_width), lambda o: (o, 0)),
            pl.BlockSpec((rows, groups * k_width), lambda o: (o, 0)),
            pl.BlockSpec((rows, groups * k_width), lambda o: (o, 0)),
            pl.BlockSpec((2 * q_width, nx * rows), lambda o: (o % ny, o // ny)),
            pl.BlockSpec((8, rows), lambda o: (o, 0)),
        ],
        out_shape=[
            jax.ShapeDtypeStruct((dim, groups * q_width), F32),
            jax.ShapeDtypeStruct((dim, groups * k_width), F32),
            jax.ShapeDtypeStruct((dim, groups * k_width), F32),
            jax.ShapeDtypeStruct((2 * ny * q_width, nz * nx * rows), F32),
            jax.ShapeDtypeStruct((8 * outer, rows), F32),
        ],
        name="spread_attn",
    )(stacked)


def solution(mesh):
    sp_size = mesh.shape["sp"]
    dp_size = mesh.shape["dp"]
    side = round(dp_size**0.5)
    grid = jax.sharding.Mesh(mesh.devices.reshape(side, dp_size // side, sp_size // 2, 2), ("z", "y", "x", "c"))
    seq_spec = P(("z", "y"), ("x", "c"), None)
    seq_axes, mlp_axes = ("x", "c"), ("y", "c")
    mlp_size = grid.shape["y"] * 2
    mlp_outer = grid.shape["z"] * grid.shape["x"]
    inv_batch = 1.0 / dp_size

    def device_step(tokens, grad_out, norm_attn, w_query, w_key, w_value, w_out, norm_mlp, w_gate, w_up, w_down):
        x = tokens[0]
        dy = grad_out[0]
        n_local, dim = x.shape
        n_seq = n_local * sp_size
        q_width = w_query.shape[1] // sp_size
        k_width = w_key.shape[1] // sp_size
        ff_local = w_gate.shape[1] // mlp_size
        rows = dim // dp_size
        attn_blk = min(512, n_seq // 2)
        cos_all, sin_all = rope_tables(jnp.arange(n_seq))

        def to_heads(stacked):
            return lax.all_to_all(stacked, seq_axes, 0, 0, tiled=True)

        def gather(local, axes):
            return lax.all_gather(local, axes, axis=0, tiled=True)

        normed, unit_attn, inv_attn = norm_fwd(x, norm_attn)
        dy_full = gather(dy, mlp_axes)
        normed_full, qkv = gather_qkv(normed, w_query, w_key, w_value, sp_size, 3)
        _, lse, attn_tok = attn_fwd(qkv, sp_size // 2, 4)
        w_out_heads = w_out.reshape(sp_size, q_width, dim)
        projected = jnp.einsum("jte,jed->td", attn_tok, w_out_heads, preferred_element_type=F32)
        hidden = (x.astype(F32) + projected).astype(BF16)
        normed_mlp, unit_mlp, inv_mlp = norm_fwd(hidden, norm_mlp)
        m_full = gather(normed_mlp, mlp_axes)

        grad_m = mlp_grad_input(normed_mlp, dy, w_gate, w_up, w_down, min(512, w_gate.shape[1]))
        grad_hid_norm, g_norm_mlp = norm_bwd(grad_m, unit_mlp, inv_mlp, norm_mlp)
        grad_hidden = (dy.astype(F32) + grad_hid_norm).astype(BF16)
        grad_hidden_y = gather(grad_hidden, mlp_axes)
        attn_y = lax.all_to_all(attn_tok, mlp_axes, 0, 0, tiled=True).reshape(n_seq, q_width)

        g_mlp = mlp_ring(m_full, dy_full, w_gate, w_up, w_down, ff_local, inv_batch, "z", "x", side, mlp_axes, 1)
        g_mlp, late_hidden = lax.optimization_barrier((g_mlp, grad_hidden))
        g_mlp = gather(g_mlp, ("z", "x", "y", "c"))

        grad_attn = jnp.einsum("td,jed->jte", late_hidden, w_out_heads, preferred_element_type=F32).astype(BF16)
        grad_attn = to_heads(grad_attn).reshape(n_seq, q_width)
        g_out = tn(grad_hidden_y, attn_y).astype(BF16).reshape(mlp_outer, rows, q_width)
        g_out = ring_reduce(g_out, inv_batch, 1, "z", "x", 5)

        gqkv = attn_bwd(qkv, grad_attn, lse, cos_all, sin_all, attn_blk)
        gqkv_tok = to_heads(gqkv.reshape(sp_size, n_local, q_width + 2 * k_width))
        flat = lambda t: jnp.transpose(t, (1, 0, 2)).reshape(n_local, -1)
        grad_normed = (
            nt(flat(gqkv_tok[:, :, :q_width]), w_query)
            + nt(flat(gqkv_tok[:, :, q_width : q_width + k_width]), w_key)
            + nt(flat(gqkv_tok[:, :, q_width + k_width :]), w_value)
        ).astype(BF16)
        grad_tok_norm, g_norm_attn = norm_bwd(grad_normed, unit_attn, inv_attn, norm_attn)
        grad_tokens = (grad_hidden.astype(F32) + grad_tok_norm).astype(BF16)

        g_attn = tn(normed_full, gqkv).astype(BF16).reshape(dp_size, rows, q_width + 2 * k_width)
        gains = jnp.stack([g_norm_attn.reshape(dp_size, rows), g_norm_mlp.reshape(dp_size, rows)], axis=1)
        gains = jnp.pad(gains.astype(BF16), ((0, 0), (0, rows - 2), (0, 0)))
        g_attn = ring_reduce(jnp.concatenate([g_attn, gains], axis=2), inv_batch, 2, "z", "y", 2)
        gain_at = q_width + 2 * k_width
        gains = jnp.pad(g_attn[:8, gain_at:], ((0, 0), (0, 2 * (q_width + k_width) - rows)))
        g_attn = jnp.concatenate([jnp.concatenate([g_attn[:, :gain_at], g_out], axis=1), gains], axis=0)
        g_attn = gather(g_attn, ("z", "y", "x", "c"))

        g_gate, g_up, g_down = spread_mlp(g_mlp, mlp_outer, mlp_size, ff_local)
        g_query, g_key, g_value, g_out, gains = spread_attn(g_attn, side, dp_size // side, sp_size, q_width, k_width)
        gains = gains.reshape(dp_size, 8, rows)
        return (
            grad_tokens[None],
            gains[:, 0].reshape(dim),
            g_query,
            g_key,
            g_value,
            g_out,
            gains[:, 1].reshape(dim),
            g_gate,
            g_up,
            g_down,
        )

    return jax.shard_map(device_step, mesh=grid, in_specs=(seq_spec, seq_spec) + (P(),) * 9, out_specs=(seq_spec,) + (P(),) * 9, check_vma=False)
```

```python
import functools
import math

import jax
import jax.numpy as jnp
from jax import lax
from jax.experimental import pallas as pl
from jax.experimental.pallas import tpu as pltpu
from jax.sharding import PartitionSpec as P


NORM_EPS = 1.0e-5
ROPE_BASE = 1.0e6
HEAD_DIM = 128
F32 = jnp.float32
BF16 = jnp.bfloat16
VMEM_LIMIT = 60 * 1024 * 1024
MESH = pl.DeviceIdType.MESH
NEG = -1.0e30


def nn(a, b):
    return lax.dot_general(a, b, (((1,), (0,)), ((), ())), preferred_element_type=F32)


def nt(a, b):
    return lax.dot_general(a, b, (((1,), (1,)), ((), ())), preferred_element_type=F32)


def tn(a, b):
    return lax.dot_general(a, b, (((0,), (0,)), ((), ())), preferred_element_type=F32)


def norm_fwd(values, gain_vec):
    values_f = values.astype(F32)
    inv_rms = lax.rsqrt(jnp.mean(values_f * values_f, axis=-1, keepdims=True) + NORM_EPS)
    unit_vals = values_f * inv_rms
    return (unit_vals * gain_vec.astype(F32)).astype(BF16), unit_vals, inv_rms


def norm_bwd(grad_normed, unit_vals, inv_rms, gain_vec):
    grad_f = grad_normed.astype(F32)
    grad_gain = jnp.sum(grad_f * unit_vals, axis=0)
    grad_unit = grad_f * gain_vec.astype(F32)
    grad_in = inv_rms * (grad_unit - unit_vals * jnp.mean(grad_unit * unit_vals, axis=-1, keepdims=True))
    return grad_in, grad_gain


def rope_tables(positions):
    half_dim = HEAD_DIM // 2
    inv_freq = ROPE_BASE ** (-jnp.arange(half_dim, dtype=F32) * (2.0 / HEAD_DIM))
    angles = positions.astype(F32)[:, None] * inv_freq[None, :]
    cos, sin = jnp.cos(angles), jnp.sin(angles)
    return jnp.concatenate([cos, cos], axis=-1), jnp.concatenate([-sin, sin], axis=-1)


def rope(values, cos_tab, sin_tab):
    return values * cos_tab + pltpu.roll(values, HEAD_DIM // 2, 1) * sin_tab


def call(kernel, flops, moved, **kwargs):
    params = pltpu.CompilerParams(vmem_limit_bytes=VMEM_LIMIT)
    cost = pl.CostEstimate(flops=int(flops), bytes_accessed=int(moved), transcendentals=0)
    return pl.pallas_call(kernel, compiler_params=params, cost_estimate=cost, **kwargs)


def whole(shape):
    return pl.BlockSpec(shape, lambda *_: (0,) * len(shape))


def gather_qkv_kernel(x_ref, wq_ref, wk_ref, wv_ref, cos_blk, sin_blk, cos_row, sin_row, full_ref, qkv_ref, land, weights, w_sems, o_sems, i_send, i_recv, d_send, d_recv):
    x, c = lax.axis_index("x"), lax.axis_index("c")
    n = land.shape[0] // 2
    tok = x_ref.shape[0]
    half = tok // 2
    qw, kw = wq_ref.shape[1] // (2 * n), wk_ref.shape[1] // (2 * n)
    width = qw + 2 * kw
    wrap = lambda v: lax.rem(v + 2 * n, n)
    at = lambda dx, core: 2 * wrap(x + dx) + core
    me = 2 * x + c

    loads = []
    for k, (ref, start, size) in enumerate(((wq_ref, 0, qw), (wk_ref, qw, kw), (wv_ref, qw + kw, kw))):
        cols = pl.ds(pl.multiple_of(me * size, 128), size)
        loads.append(pltpu.make_async_copy(ref.at[:, cols], weights.at[:, pl.ds(start, size)], w_sems.at[k]))
        loads[-1].start()

    barrier = pltpu.get_barrier_semaphore()
    for goal in ({"x": wrap(x + 1)}, {"x": wrap(x - 1)}, {"c": 1 - c}):
        pl.semaphore_signal(barrier, inc=1, device_id=goal, device_id_type=MESH)
    pl.semaphore_wait(barrier, 3)

    rows = lambda h: pl.ds(h * half, half)

    def ring(way, hop, h):
        k = (0 if way > 0 else 3) + (h if hop == 0 else 2)
        src = land.at[at(-way * hop, c), rows(h)] if hop else x_ref.at[rows(h)]
        dst = land.at[at(-way * hop, c), rows(h)]
        return pltpu.make_async_remote_copy(src, dst, i_send.at[k], i_recv.at[k], device_id={"x": wrap(x + way)}, device_id_type=MESH)

    def across(k, dx, h):
        part = rows(h) if h is not None else pl.ds(0, tok)
        src = land.at[at(dx, c), part] if dx else x_ref.at[part]
        return pltpu.make_async_remote_copy(src, land.at[at(dx, c), part], d_send.at[k], d_recv.at[k], device_id={"c": 1 - c}, device_id_type=MESH)

    first = [ring(1, 0, 0), ring(-1, 0, 1), ring(1, 0, 1), ring(-1, 0, 0)]
    second = [ring(1, 1, 0), ring(-1, 1, 1)]
    die = [across(0, 0, None), across(1, -1, 0), across(2, 1, 1), across(3, -1, 1), across(4, 1, 0), across(5, 2, 0), across(6, 2, 1)]
    for copy in first[:2] + die[:1] + first[2:]:
        copy.start()
    land[me] = x_ref[...]
    for load in loads:
        load.wait()

    def wait_block(k):
        @pl.when(k == 1)
        def _():
            die[0].wait_recv()

        @pl.when(k == 2)
        def _():
            first[0].wait_recv()
            second[0].start()
            die[1].start()
            first[1].wait_recv()
            second[1].start()
            die[2].start()
            first[2].wait_recv()
            die[3].start()

        @pl.when(k == 3)
        def _():
            first[3].wait_recv()
            die[4].start()

        @pl.when(k == 4)
        def _():
            die[1].wait_recv()
            die[3].wait_recv()

        @pl.when(k == 5)
        def _():
            die[2].wait_recv()
            die[4].wait_recv()

        @pl.when(k == 6)
        def _():
            second[0].wait_recv()
            die[5].start()
            second[1].wait_recv()
            die[6].start()

        @pl.when(k == 7)
        def _():
            die[5].wait_recv()
            die[6].wait_recv()

    def out_copy(k):
        dx = jnp.where(k < 2, 0, jnp.where(k >= 6, 2, jnp.where(lax.rem(k, 2) == 0, -1, 1)))
        core = jnp.where((k == 1) | (k == 4) | (k == 5) | (k == 7), 1 - c, c)
        block = 2 * wrap(x + dx) + core
        here = pl.ds(pl.multiple_of(block * tok, tok), tok)
        return block, here, pltpu.make_async_copy(land.at[block], full_ref.at[here, :], o_sems.at[k])

    def body(k, carry):
        wait_block(k)
        block, here, copy = out_copy(k)
        copy.start()
        value = nn(land[block], weights[...])
        cos_b, sin_b = cos_blk[pl.ds(block, 1), :], sin_blk[pl.ds(block, 1), :]
        cos = cos_b * cos_row[...] - sin_b * sin_row[...]
        sin = sin_b * cos_row[...] + cos_b * sin_row[...]
        for start in range(0, width, HEAD_DIM):
            part = value[:, start : start + HEAD_DIM]
            if start < qw + kw:
                part = rope(part, cos, sin)
            qkv_ref[here, start : start + HEAD_DIM] = part.astype(BF16)
        return carry

    lax.fori_loop(0, 2 * n, body, 0)
    for copy in first + second + die:
        copy.wait_send()
    for k in range(2 * n):
        out_copy(k)[2].wait()


def gather_qkv(normed, w_query, w_key, w_value, groups, collective_id):
    tok, dim = normed.shape
    width = (w_query.shape[1] + w_key.shape[1] + w_value.shape[1]) // groups
    anywhere = pl.BlockSpec(memory_space=pl.ANY)
    vmem = pl.BlockSpec(memory_space=pltpu.VMEM)
    return pl.pallas_call(
        gather_qkv_kernel,
        in_specs=[vmem, anywhere, anywhere, anywhere, vmem, vmem, vmem, vmem],
        out_specs=[anywhere, vmem],
        out_shape=[jax.ShapeDtypeStruct((groups * tok, dim), BF16), jax.ShapeDtypeStruct((groups * tok, width), BF16)],
        scratch_shapes=[
            pltpu.VMEM((groups, tok, dim), BF16),
            pltpu.VMEM((dim, width), BF16),
            pltpu.SemaphoreType.DMA((3,)),
            pltpu.SemaphoreType.DMA((groups,)),
            pltpu.SemaphoreType.DMA((6,)),
            pltpu.SemaphoreType.DMA((6,)),
            pltpu.SemaphoreType.DMA((7,)),
            pltpu.SemaphoreType.DMA((7,)),
        ],
        compiler_params=pltpu.CompilerParams(collective_id=collective_id, has_side_effects=True, vmem_limit_bytes=VMEM_LIMIT),
        cost_estimate=pl.CostEstimate(flops=20_000_000_000, bytes_accessed=6 * groups * tok * dim, transcendentals=0),
        name="gather_qkv",
    )(normed, w_query, w_key, w_value, *rope_tables(jnp.arange(groups) * tok), *rope_tables(jnp.arange(tok)))


def attn_fwd_kernel(blk, n_q, qkv_ref, out_ref, lse_ref, tok_ref, mine, land, send_sems, recv_sems, *scrs):
    step, steps = pl.program_id(0), pl.num_programs(0)
    x, c = lax.axis_index("x"), lax.axis_index("c")
    me = 2 * x + c
    tok = blk // 2

    def block_of(step):
        ahead = jnp.where(step == 0, 2, jnp.where(step == 1, 1, jnp.where(step == 2, steps - 1, 0)))
        return lax.rem(x + ahead, steps)

    def send(step, core):
        goal = block_of(step)
        src = mine.at[2 * goal + core]
        return pltpu.make_async_remote_copy(src, land.at[me], send_sems.at[step, core], recv_sems.at[me], device_id={"x": goal, "c": core}, device_id_type=MESH)

    @pl.when(step == 0)
    def _():
        barrier = pltpu.get_barrier_semaphore()
        for k in range(1, 2 * steps):
            peer = lax.rem(me + k, 2 * steps)
            pl.semaphore_signal(barrier, inc=1, device_id={"x": peer // 2, "c": lax.rem(peer, 2)}, device_id_type=MESH)
        pl.semaphore_wait(barrier, 2 * steps - 1)

    @pl.when(step > 0)
    def _():
        send(step - 1, 0).start()
        send(step - 1, 1).start()

    i = block_of(step)
    coef = HEAD_DIM**-0.5 * math.log2(math.e)
    k_at, v_at = n_q * HEAD_DIM, (n_q + 1) * HEAD_DIM
    at = lambda j: pl.ds(pl.multiple_of(j * blk, blk), blk)
    lanes = lambda t, op: functools.reduce(op, [t[:, s : s + 128] for s in range(0, blk, 128)])
    qs = [qkv_ref[at(i), h * HEAD_DIM : (h + 1) * HEAD_DIM] for h in range(n_q)]
    causal = lax.broadcasted_iota(jnp.int32, (blk, blk), 0) >= lax.broadcasted_iota(jnp.int32, (blk, blk), 1)

    def score_step(j, tops, masked):
        key = qkv_ref[at(j), k_at:v_at]
        new = []
        for h in range(n_q):
            s = nt(qs[h], key)
            if masked:
                s = jnp.where(causal, s, NEG)
            scrs[h][:, at(j)] = s
            new.append(jnp.maximum(tops[h], lanes(s, jnp.maximum)))
        return tuple(new)

    start = tuple(jnp.full((blk, 128), NEG, F32) for _ in range(n_q))
    tops = lax.fori_loop(0, i, lambda j, t: score_step(j, t, False), start)
    tops = score_step(i, tops, True)
    row_max = [jnp.max(t, axis=1, keepdims=True) for t in tops]

    def exp_step(j, sums):
        new = []
        for h in range(n_q):
            e = jnp.exp2((scrs[h][:, at(j)] - row_max[h]) * coef)
            scrs[h][:, at(j)] = e
            new.append(sums[h] + lanes(e, jnp.add))
        return tuple(new)

    sums = lax.fori_loop(0, i + 1, exp_step, tuple(jnp.zeros((blk, 128), F32) for _ in range(n_q)))
    row_sum = [jnp.sum(t, axis=1, keepdims=True) for t in sums]
    inv_sum = [1.0 / t for t in row_sum]

    def out_step(j, accs):
        value = qkv_ref[at(j), v_at : v_at + HEAD_DIM]
        return tuple(accs[h] + nn((scrs[h][:, at(j)] * inv_sum[h]).astype(BF16), value) for h in range(n_q))

    accs = lax.fori_loop(0, i + 1, out_step, tuple(jnp.zeros((blk, HEAD_DIM), F32) for _ in range(n_q)))
    for h in range(n_q):
        value = accs[h].astype(BF16)
        out_ref[at(i), h * HEAD_DIM : (h + 1) * HEAD_DIM] = value
        for core in range(2):
            mine[2 * i + core, :, h * HEAD_DIM : (h + 1) * HEAD_DIM] = value[core * tok : (core + 1) * tok, :]
        log_norm = row_max[h] * coef + jnp.log2(row_sum[h])
        lse_ref[h * 8 : (h + 1) * 8, at(i)] = jnp.transpose(jnp.broadcast_to(log_norm, (blk, 128)))[:8, :]

    @pl.when(step == steps - 1)
    def _():
        land[me] = mine[me]
        send(step, 1 - c).start()
        for k in range(1, 2 * steps):
            peer = lax.rem(me + k, 2 * steps)
            pltpu.make_async_remote_copy(mine.at[peer], land.at[peer], send_sems.at[0, 0], recv_sems.at[peer], device_id={"x": x, "c": c}, device_id_type=MESH).wait_recv()
        tok_ref[...] = land[...]
        for k in range(steps - 1):
            send(k, 0).wait_send()
            send(k, 1).wait_send()
        send(step, 1 - c).wait_send()


def attn_fwd(qkv, steps, collective_id):
    seq, width = qkv.shape
    n_q = width // HEAD_DIM - 2
    blk = seq // steps
    return pl.pallas_call(
        functools.partial(attn_fwd_kernel, blk, n_q),
        grid=(steps,),
        in_specs=[whole((seq, width))],
        out_specs=[whole((seq, n_q * HEAD_DIM)), whole((8 * n_q, seq)), whole((2 * steps, blk // 2, n_q * HEAD_DIM))],
        out_shape=[
            jax.ShapeDtypeStruct((seq, n_q * HEAD_DIM), BF16),
            jax.ShapeDtypeStruct((8 * n_q, seq), F32),
            jax.ShapeDtypeStruct((2 * steps, blk // 2, n_q * HEAD_DIM), BF16),
        ],
        scratch_shapes=[pltpu.VMEM((2 * steps, blk // 2, n_q * HEAD_DIM), BF16)] * 2
        + [pltpu.SemaphoreType.DMA((steps, 2)), pltpu.SemaphoreType.DMA((2 * steps,))]
        + [pltpu.VMEM((blk, seq), F32)] * n_q,
        compiler_params=pltpu.CompilerParams(collective_id=collective_id, has_side_effects=True, vmem_limit_bytes=VMEM_LIMIT),
        cost_estimate=pl.CostEstimate(flops=2 * n_q * seq * seq * HEAD_DIM * 2, bytes_accessed=seq * width * 2, transcendentals=0),
        name="attn_fwd",
    )(qkv)


def attn_bwd_kernel(blk, n_q, qkv_ref, do_ref, lse_ref, cos_blk, sin_blk, cos_row, sin_row, out_ref, dk_scr, dv_scr, *scrs):
    i, steps = pl.program_id(0), pl.num_programs(0)
    scale = HEAD_DIM**-0.5
    coef = scale * math.log2(math.e)
    k_at, v_at = n_q * HEAD_DIM, (n_q + 1) * HEAD_DIM
    at = lambda j: pl.ds(pl.multiple_of(j * blk, blk), blk)
    p_scrs, dp_scrs = scrs[:n_q], scrs[n_q:]
    qs = [qkv_ref[at(i), h * HEAD_DIM : (h + 1) * HEAD_DIM] for h in range(n_q)]
    dos = [do_ref[:, h * HEAD_DIM : (h + 1) * HEAD_DIM] for h in range(n_q)]
    lses = [lse_ref[h * 8 : h * 8 + 1, :] for h in range(n_q)]
    causal = lax.broadcasted_iota(jnp.int32, (blk, blk), 0) <= lax.broadcasted_iota(jnp.int32, (blk, blk), 1)

    @pl.when(i == 0)
    def _():
        dk_scr[...] = jnp.zeros_like(dk_scr)
        dv_scr[...] = jnp.zeros_like(dv_scr)

    def prob_step(j, dots):
        key, value = qkv_ref[at(j), k_at:v_at], qkv_ref[at(j), v_at : v_at + HEAD_DIM]
        new, dv = [], dv_scr[at(j), :]
        for h in range(n_q):
            p = jnp.where(causal | (j < i), jnp.exp2(nt(key, qs[h]) * coef - lses[h]), 0.0)
            dp = nt(value, dos[h]).astype(BF16)
            p_scrs[h][at(j), :] = p
            dp_scrs[h][at(j), :] = dp
            dv = dv + nn(p.astype(BF16), dos[h])
            new.append(dots[h] + jnp.sum((p * dp.astype(F32)).reshape(blk // 8, 8, blk), axis=0))
        dv_scr[at(j), :] = dv
        return tuple(new)

    dots = lax.fori_loop(0, i + 1, prob_step, tuple(jnp.zeros((8, blk), F32) for _ in range(n_q)))
    row_dot = [jnp.sum(t, axis=0, keepdims=True) for t in dots]

    def grad_step(j, accs):
        key = qkv_ref[at(j), k_at:v_at]
        new, dk = [], dk_scr[at(j), :]
        for h in range(n_q):
            ds = (p_scrs[h][at(j), :] * (dp_scrs[h][at(j), :].astype(F32) - row_dot[h]) * scale).astype(BF16)
            dk = dk + nn(ds, qs[h])
            new.append(accs[h] + tn(ds, key))
        dk_scr[at(j), :] = dk
        return tuple(new)

    accs = lax.fori_loop(0, i + 1, grad_step, tuple(jnp.zeros((blk, HEAD_DIM), F32) for _ in range(n_q)))

    def unrope(grad, j):
        cos_b, sin_b = cos_blk[pl.ds(j, 1), :], sin_blk[pl.ds(j, 1), :]
        cos = cos_b * cos_row[...] - sin_b * sin_row[...]
        sin = sin_b * cos_row[...] + cos_b * sin_row[...]
        return rope(grad.astype(BF16).astype(F32), cos, -sin).astype(BF16)

    for h in range(n_q):
        out_ref[at(i), h * HEAD_DIM : (h + 1) * HEAD_DIM] = unrope(accs[h], i)

    @pl.when(i == steps - 1)
    def _():
        def finish(j, carry):
            out_ref[at(j), k_at:v_at] = unrope(dk_scr[at(j), :], j)
            out_ref[at(j), v_at : v_at + HEAD_DIM] = dv_scr[at(j), :].astype(BF16)
            return carry

        lax.fori_loop(0, steps, finish, 0)


def attn_bwd(qkv, grad_out, lse, blk):
    seq, width = qkv.shape
    n_q = width // HEAD_DIM - 2
    return call(
        functools.partial(attn_bwd_kernel, blk, n_q),
        5 * n_q * seq * seq * HEAD_DIM * 2,
        seq * width * 4,
        grid=(seq // blk,),
        in_specs=[
            whole((seq, width)),
            pl.BlockSpec((blk, n_q * HEAD_DIM), lambda i: (i, 0)),
            pl.BlockSpec((8 * n_q, blk), lambda i: (0, i)),
            whole((seq // blk, HEAD_DIM)),
            whole((seq // blk, HEAD_DIM)),
            whole((blk, HEAD_DIM)),
            whole((blk, HEAD_DIM)),
        ],
        out_specs=whole((seq, width)),
        out_shape=jax.ShapeDtypeStruct((seq, width), BF16),
        scratch_shapes=[pltpu.VMEM((seq, HEAD_DIM), F32)] * 2
        + [pltpu.VMEM((seq, blk), F32)] * n_q
        + [pltpu.VMEM((seq, blk), BF16)] * n_q,
        name="attn_bwd",
    )(qkv, grad_out, lse, *rope_tables(jnp.arange(seq // blk) * blk), *rope_tables(jnp.arange(blk)))


def outer_kernel(a_ref, b_ref, out_ref):
    out_ref[...] = tn(a_ref[...], b_ref[...]).astype(BF16)


def outer(a, b):
    seq, dim = a.shape
    width = b.shape[1]
    tile = min(512, dim)
    return call(
        outer_kernel,
        2 * seq * dim * width,
        2 * seq * dim,
        grid=(dim // tile,),
        in_specs=[pl.BlockSpec((seq, tile), lambda i: (0, i)), whole((seq, width))],
        out_specs=pl.BlockSpec((tile, width), lambda i: (i, 0)),
        out_shape=jax.ShapeDtypeStruct((dim, width), BF16),
        name="outer",
    )(a, b)


def heads_kernel(a_ref, w_ref, out_ref):
    out_ref[0] = nt(a_ref[...], w_ref[...]).astype(BF16)


def to_head_groups(a, w, groups):
    tok, dim = a.shape
    width = w.shape[0] // groups
    return call(
        heads_kernel,
        2 * tok * dim * w.shape[0],
        2 * dim * w.shape[0],
        grid=(groups,),
        in_specs=[whole((tok, dim)), pl.BlockSpec((width, dim), lambda j: (j, 0))],
        out_specs=pl.BlockSpec((1, tok, width), lambda j: (j, 0, 0)),
        out_shape=jax.ShapeDtypeStruct((groups, tok, width), BF16),
        name="to_head_groups",
    )(a, w)


def from_heads_kernel(g_ref, wq_ref, wk_ref, wv_ref, out_ref, acc_ref):
    step = pl.program_id(0)
    qw = wq_ref.shape[1]
    grad = g_ref[0]
    total = nt(grad[:, :qw], wq_ref[...]) + nt(grad[:, qw:], jnp.concatenate([wk_ref[...], wv_ref[...]], axis=1))

    @pl.when(step == 0)
    def _():
        acc_ref[...] = total

    @pl.when(step > 0)
    def _():
        acc_ref[...] += total

    @pl.when(step == pl.num_programs(0) - 1)
    def _():
        out_ref[...] = acc_ref[...].astype(BF16)


def from_head_groups(grads, w_query, w_key, w_value):
    groups, tok, width = grads.shape
    dim = w_query.shape[0]
    qw, kw = w_query.shape[1] // groups, w_key.shape[1] // groups
    return call(
        from_heads_kernel,
        2 * tok * dim * width * groups,
        2 * dim * width * groups,
        grid=(groups,),
        in_specs=[
            pl.BlockSpec((1, tok, width), lambda j: (j, 0, 0)),
            pl.BlockSpec((dim, qw), lambda j: (0, j)),
            pl.BlockSpec((dim, kw), lambda j: (0, j)),
            pl.BlockSpec((dim, kw), lambda j: (0, j)),
        ],
        out_specs=whole((tok, dim)),
        out_shape=jax.ShapeDtypeStruct((tok, dim), BF16),
        scratch_shapes=[pltpu.VMEM((tok, dim), F32)],
        name="from_head_groups",
    )(grads, w_query, w_key, w_value)


def act_grads(gate, up, grad_act):
    sig = 1.0 / (1.0 + jnp.exp(-gate))
    act = gate * sig
    grad_gate = (grad_act * up * sig * (1.0 + gate * (1.0 - sig))).astype(BF16)
    grad_up = (grad_act * act).astype(BF16)
    return (act * up).astype(BF16), grad_gate, grad_up


def mlp_kernel(m_ref, dy_ref, wg_ref, wu_ref, wd_ref, out_ref, acc_ref):
    step = pl.program_id(0)
    m, dy = m_ref[...], dy_ref[...]
    grad_act = nt(dy, wd_ref[...]).astype(BF16).astype(F32)
    _, grad_gate, grad_up = act_grads(nn(m, wg_ref[...]), nn(m, wu_ref[...]), grad_act)
    total = nt(grad_gate, wg_ref[...]) + nt(grad_up, wu_ref[...])

    @pl.when(step == 0)
    def _():
        acc_ref[...] = total

    @pl.when(step > 0)
    def _():
        acc_ref[...] += total

    @pl.when(step == pl.num_programs(0) - 1)
    def _():
        out_ref[...] = acc_ref[...].astype(BF16)


def mlp_grad_input(m, dy, w_gate, w_up, w_down, blk):
    tok, dim = m.shape
    width = w_gate.shape[1]
    return call(
        mlp_kernel,
        5 * 2 * tok * dim * width,
        3 * 2 * dim * width,
        grid=(width // blk,),
        in_specs=[
            whole((tok, dim)),
            whole((tok, dim)),
            pl.BlockSpec((dim, blk), lambda j: (0, j)),
            pl.BlockSpec((dim, blk), lambda j: (0, j)),
            pl.BlockSpec((blk, dim), lambda j: (j, 0)),
        ],
        out_specs=whole((tok, dim)),
        out_shape=jax.ShapeDtypeStruct((tok, dim), BF16),
        scratch_shapes=[pltpu.VMEM((tok, dim), F32)],
        name="mlp_grad_input",
    )(m, dy, w_gate, w_up, w_down)


class Ring:
    def __init__(self, n, subs, slow, fast, source, recv1, acc, send2, recv2, s1, r1, s2, r2):
        self.n, self.subs, self.slow, self.fast, self.source = n, subs, slow, fast, source
        self.recv1, self.acc, self.send2, self.recv2 = recv1, acc, send2, recv2
        self.s1, self.r1, self.s2, self.r2 = s1, r1, s2, r2
        self.z, self.y = lax.axis_index(slow), lax.axis_index(fast)
        self.height = recv1.shape[5]

    def wrap(self, v):
        return lax.rem(v + 2 * self.n, self.n)

    def goal(self, c, phase):
        step = 1 - 2 * (c % 2)
        if (c < 2) == (phase == 1):
            return {self.fast: self.wrap(self.y + step)}
        return {self.slow: self.wrap(self.z + step)}

    def arrive(self):
        barrier = pltpu.get_barrier_semaphore()
        for c in range(4):
            pl.semaphore_signal(barrier, inc=1, device_id=self.goal(c, 1), device_id_type=MESH)

    def meet(self):
        pl.semaphore_wait(pltpu.get_barrier_semaphore(), 4)

    def coord(self, c, phase):
        return self.y if (c < 2) == (phase == 1) else self.z

    def rows(self, c, s):
        return pl.ds((c * self.subs + s) * self.height, self.height)

    def local(self, b, c, a, s):
        source = self.source(b)
        return source.at[:, a, self.rows(c, s), :] if c < 2 else source.at[a, :, self.rows(c, s), :]

    def chunk(self, c, phase, t):
        return self.wrap(self.coord(c, phase) - (1 - 2 * (c % 2)) * t)

    def copy1(self, b, c, t, s):
        src = self.recv1.at[b, c, t - 1, s] if t else self.local(b, c, self.chunk(c, 1, 1), s)
        dst = self.recv1.at[b, c, t, s]
        return pltpu.make_async_remote_copy(src, dst, self.s1.at[b, c, t, s], self.r1.at[b, c, t, s], device_id=self.goal(c, 1), device_id_type=MESH)

    def copy2(self, b, c, t, s):
        src = self.recv2.at[b, c, t - 1, s] if t else self.send2.at[b, c, s]
        dst = self.recv2.at[b, c, t, s]
        return pltpu.make_async_remote_copy(src, dst, self.s2.at[b, c, t, s], self.r2.at[b, c, t, s], device_id=self.goal(c, 2), device_id_type=MESH)

    def start(self, b):
        for s in range(self.subs):
            for c in range(4):
                self.copy1(b, c, 0, s).start()

    def hop1(self, b, t):
        for s in range(self.subs):
            for c in range(4):
                self.copy1(b, c, t, s).wait_recv()
                mine = self.local(b, c, self.chunk(c, 1, t + 2), s)[...]
                total = self.recv1[b, c, t, s].astype(F32) + mine.astype(F32)
                if t < self.n - 2:
                    self.recv1[b, c, t, s] = total.astype(BF16)
                    self.copy1(b, c, t + 1, s).start()
                else:
                    self.acc[b, c, s] = total
                    self.send2[b, c, s] = self.acc[b, c, s, self.chunk(c, 2, 1)].astype(BF16)
                    self.copy2(b, c, 0, s).start()

    def hop2(self, b, t, scale, store):
        for s in range(self.subs):
            for c in range(4):
                self.copy2(b, c, t, s).wait_recv()
                total = self.recv2[b, c, t, s].astype(F32) + self.acc[b, c, s, self.chunk(c, 2, t + 2)]
                if t < self.n - 2:
                    self.recv2[b, c, t, s] = total.astype(BF16)
                    self.copy2(b, c, t + 1, s).start()
                else:
                    store(b, (c * self.subs + s) * self.height, self.height, (total * scale).astype(BF16))

    def drain(self, b):
        for s in range(self.subs):
            for c in range(4):
                for t in range(self.n - 1):
                    self.copy1(b, c, t, s).wait_send()
                    self.copy2(b, c, t, s).wait_send()

    @staticmethod
    def scratch(n, blocks, subs, rows, width):
        height = rows // (4 * subs)
        return [
            pltpu.VMEM((blocks, 4, n - 1, subs, n, height, width), BF16),
            pltpu.VMEM((blocks, 4, subs, n, height, width), F32),
            pltpu.VMEM((blocks, 4, subs, height, width), BF16),
            pltpu.VMEM((blocks, 4, n - 1, subs, height, width), BF16),
        ] + [pltpu.SemaphoreType.DMA((blocks, 4, n - 1, subs))] * 4


def mlp_ring_kernel(n, subs, scale, blocks, slow, fast, group, m_all, dy_all, wg_all, wu_all, wd_all, out_ref, m_ref, dy_ref, in_sems, wg_buf, wu_buf, wd_buf, w_sems, grads_ref, act_ref, g_ref, *scratch):
    step = pl.program_id(0)
    seq, dim = m_ref.shape
    width = act_ref.shape[0]
    rows = dim // (n * n)
    tiles = 4
    blk, tile = seq // tiles, dim // tiles
    per_tile = tile // rows
    ring = Ring(n, subs, slow, fast, lambda b: g_ref.at[b], *scratch)
    at = lambda i, size: pl.ds(pl.multiple_of(i * size, size), size)

    def loads(b):
        mine = at((lax.axis_index(group) if group else 0) * blocks + b, width)
        slot = lax.rem(b, 2)
        return [
            pltpu.make_async_copy(wg_all.at[:, mine], wg_buf.at[slot], w_sems.at[slot, 0]),
            pltpu.make_async_copy(wu_all.at[:, mine], wu_buf.at[slot], w_sems.at[slot, 1]),
            pltpu.make_async_copy(wd_all.at[mine, :], wd_buf.at[slot], w_sems.at[slot, 2]),
        ]

    def tokens(i):
        return [
            pltpu.make_async_copy(m_all.at[at(i, blk), :], m_ref.at[at(i, blk), :], in_sems.at[0, i]),
            pltpu.make_async_copy(dy_all.at[at(i, blk), :], dy_ref.at[at(i, blk), :], in_sems.at[1, i]),
        ]

    @pl.when(step == 0)
    def _():
        for load in loads(0) + [load for i in range(tiles) for load in tokens(i)]:
            load.start()
        ring.arrive()
        ring.meet()

    @pl.when(step + 1 < blocks)
    def _():
        for load in loads(step + 1):
            load.start()

    for load in loads(step):
        load.wait()
    wg_ref, wu_ref, wd_ref = (buf.at[lax.rem(step, 2)] for buf in (wg_buf, wu_buf, wd_buf))

    def store(b, first, height, value):
        out_ref[pl.ds(pl.multiple_of(b * 3 * width + first, height), height), :] = value

    hops = [functools.partial(ring.hop1, t=t) for t in range(n - 1)]
    hops += [functools.partial(ring.hop2, t=t, scale=scale, store=store) for t in range(n - 1)]
    slots = 2 * tiles
    delays = [3 * t + 3 if t < n - 1 else 3 * n - 1 + 2 * (t - n + 1) for t in range(2 * (n - 1))]

    def events(slot):
        for hop, delay in zip(hops, delays):
            since = slot - delay
            block = since // slots - 1

            @pl.when((since >= slots) & (lax.rem(since, slots) == 0) & (block < blocks))
            def _(hop=hop, block=block):
                hop(block)

    def forward(i):
        @pl.when(step == 0)
        def _():
            for load in tokens(i):
                load.wait()

        m, dy = m_ref[at(i, blk), :], dy_ref[at(i, blk), :]
        grad_act = nt(dy, wd_ref[...]).astype(BF16).astype(F32)
        act, grad_gate, grad_up = act_grads(nn(m, wg_ref[...]), nn(m, wu_ref[...]), grad_act)
        act_ref[:, at(i, blk)] = jnp.transpose(act)
        grads_ref[:width, at(i, blk)] = jnp.transpose(grad_gate)
        grads_ref[width:, at(i, blk)] = jnp.transpose(grad_up)

    def weights(i):
        grads = nn(grads_ref[...], m_ref[:, at(i, tile)]).astype(BF16)
        down = nn(act_ref[...], dy_ref[:, at(i, tile)]).astype(BF16)
        for k in range(per_tile):
            piece = i * per_tile + k
            g_ref[step, piece // n, lax.rem(piece, n), : 2 * width, :] = grads[:, k * rows : (k + 1) * rows]
            g_ref[step, piece // n, lax.rem(piece, n), 2 * width :, :] = down[:, k * rows : (k + 1) * rows]

    def slot_body(i, carry):
        @pl.when(i < tiles)
        def _():
            forward(i)

        @pl.when((i >= tiles) & (i < slots))
        def _():
            weights(i - tiles)

        events(step * slots + i)

        @pl.when(i == slots - 1)
        def _():
            ring.start(step)

        return carry

    last = step == blocks - 1
    lax.fori_loop(0, jnp.where(last, 2 * slots + max(delays), slots), slot_body, 0)

    @pl.when(last)
    def _():
        def drain(b, carry):
            ring.drain(b)
            return carry

        lax.fori_loop(0, blocks, drain, 0)


def mlp_ring(m, dy, w_gate, w_up, w_down, ff, scale, slow, fast, n, group, collective_id):
    seq, dim = m.shape
    width = min(256, ff)
    blocks = ff // width
    subs = 2
    rows = dim // (n * n)
    anywhere = pl.BlockSpec(memory_space=pl.ANY)
    return pl.pallas_call(
        functools.partial(mlp_ring_kernel, n, subs, scale, blocks, slow, fast, group),
        grid=(blocks,),
        in_specs=[anywhere] * 5,
        out_specs=pl.BlockSpec((3 * ff, rows), lambda j: (0, 0)),
        scratch_shapes=[
            pltpu.VMEM((seq, dim), BF16),
            pltpu.VMEM((seq, dim), BF16),
            pltpu.SemaphoreType.DMA((2, 4)),
            pltpu.VMEM((2, dim, width), BF16),
            pltpu.VMEM((2, dim, width), BF16),
            pltpu.VMEM((2, width, dim), BF16),
            pltpu.SemaphoreType.DMA((2, 3)),
            pltpu.VMEM((2 * width, seq), BF16),
            pltpu.VMEM((width, seq), BF16),
            pltpu.VMEM((blocks, n, n, 3 * width, rows), BF16),
        ]
        + Ring.scratch(n, blocks, subs, 3 * width, rows),
        out_shape=jax.ShapeDtypeStruct((3 * ff, rows), BF16),
        compiler_params=pltpu.CompilerParams(collective_id=collective_id, has_side_effects=True, vmem_limit_bytes=VMEM_LIMIT),
        cost_estimate=pl.CostEstimate(flops=18 * seq * dim * ff, bytes_accessed=4 * seq * dim, transcendentals=0),
        name="mlp_ring",
    )(m, dy, w_gate, w_up, w_down)


def ring_reduce_kernel(n, subs, scale, slow, fast, g_ref, out_ref, *scratch):
    ring = Ring(n, subs, slow, fast, lambda b: g_ref, *scratch)

    def store(b, first, height, value):
        out_ref[first : first + height, :] = value

    ring.arrive()
    ring.meet()
    ring.start(0)
    for t in range(n - 1):
        ring.hop1(0, t)
    for t in range(n - 1):
        ring.hop2(0, t, scale, store)
    ring.drain(0)


def ring_reduce(pieces, scale, subs, slow, fast, collective_id):
    total, rows, width = pieces.shape
    n = round(total**0.5)
    return pl.pallas_call(
        functools.partial(ring_reduce_kernel, n, subs, scale, slow, fast),
        out_shape=jax.ShapeDtypeStruct((rows, width), BF16),
        in_specs=[pl.BlockSpec(memory_space=pltpu.VMEM)],
        out_specs=pl.BlockSpec(memory_space=pltpu.VMEM),
        scratch_shapes=Ring.scratch(n, 1, subs, rows, width),
        compiler_params=pltpu.CompilerParams(collective_id=collective_id, has_side_effects=True, vmem_limit_bytes=VMEM_LIMIT),
        cost_estimate=pl.CostEstimate(flops=40_000_000_000, bytes_accessed=2 * total * rows * width, transcendentals=0),
        name="ring_reduce",
    )(pieces.reshape(n, n, rows, width))


def spread_mlp_kernel(groups, ff_local, width, in_ref, gate_ref, up_ref, down_ref):
    for g in range(groups):
        for at in range(g * ff_local, (g + 1) * ff_local, width):
            gate_ref[:, at : at + width] = jnp.transpose(in_ref[3 * at : 3 * at + width, :]).astype(F32)
            up_ref[:, at : at + width] = jnp.transpose(in_ref[3 * at + width : 3 * at + 2 * width, :]).astype(F32)
            down_ref[at : at + width, :] = in_ref[3 * at + 2 * width : 3 * at + 3 * width, :].astype(F32)


def spread_mlp(stacked, outer, groups, ff_local):
    total, rows = stacked.shape
    ff, dim = ff_local * groups, rows * outer
    return call(
        functools.partial(spread_mlp_kernel, groups, ff_local, min(256, ff_local)),
        total * rows,
        total * rows * 6,
        grid=(outer,),
        in_specs=[pl.BlockSpec((total // outer, rows), lambda o: (o, 0))],
        out_specs=[
            pl.BlockSpec((rows, ff), lambda o: (o, 0)),
            pl.BlockSpec((rows, ff), lambda o: (o, 0)),
            pl.BlockSpec((ff, rows), lambda o: (0, o)),
        ],
        out_shape=[jax.ShapeDtypeStruct((dim, ff), F32)] * 2 + [jax.ShapeDtypeStruct((ff, dim), F32)],
        name="spread_mlp",
    )(stacked)


def spread_attn_kernel(groups, q_width, k_width, in_ref, q_ref, k_ref, v_ref, o_ref, gain_ref):
    rows = q_ref.shape[0]
    gain = None
    for g in range(groups):
        first = g * (rows + 8)
        piece = in_ref[first : first + rows, :].astype(F32)
        q_ref[:, g * q_width : (g + 1) * q_width] = piece[:, :q_width]
        k_ref[:, g * k_width : (g + 1) * k_width] = piece[:, q_width : q_width + k_width]
        v_ref[:, g * k_width : (g + 1) * k_width] = piece[:, q_width + k_width : q_width + 2 * k_width]
        block, core = g // 2, g % 2
        o_ref[core * q_width : (core + 1) * q_width, block * rows : (block + 1) * rows] = jnp.transpose(piece[:, q_width + 2 * k_width :])
        part = in_ref[first + rows : first + rows + 8, :rows].astype(F32)
        gain = part if gain is None else gain + part
    gain_ref[...] = gain


def spread_attn(stacked, nz, ny, groups, q_width, k_width):
    total, row_width = stacked.shape
    outer = nz * ny
    rows = total // (outer * groups) - 8
    dim = rows * outer
    nx = groups // 2
    return call(
        functools.partial(spread_attn_kernel, groups, q_width, k_width),
        total * row_width,
        total * row_width * 6,
        grid=(outer,),
        in_specs=[pl.BlockSpec((total // outer, row_width), lambda o: (o, 0))],
        out_specs=[
            pl.BlockSpec((rows, groups * q_width), lambda o: (o, 0)),
            pl.BlockSpec((rows, groups * k_width), lambda o: (o, 0)),
            pl.BlockSpec((rows, groups * k_width), lambda o: (o, 0)),
            pl.BlockSpec((2 * q_width, nx * rows), lambda o: (o % ny, o // ny)),
            pl.BlockSpec((8, rows), lambda o: (o, 0)),
        ],
        out_shape=[
            jax.ShapeDtypeStruct((dim, groups * q_width), F32),
            jax.ShapeDtypeStruct((dim, groups * k_width), F32),
            jax.ShapeDtypeStruct((dim, groups * k_width), F32),
            jax.ShapeDtypeStruct((2 * ny * q_width, nz * nx * rows), F32),
            jax.ShapeDtypeStruct((8 * outer, rows), F32),
        ],
        name="spread_attn",
    )(stacked)


def solution(mesh):
    sp_size = mesh.shape["sp"]
    dp_size = mesh.shape["dp"]
    side = round(dp_size**0.5)
    grid = jax.sharding.Mesh(mesh.devices.reshape(side, dp_size // side, sp_size // 2, 2), ("z", "y", "x", "c"))
    seq_spec = P(("z", "y"), ("x", "c"), None)
    seq_axes, mlp_axes = ("x", "c"), ("y", "c")
    mlp_size = grid.shape["y"] * 2
    mlp_outer = grid.shape["z"] * grid.shape["x"]
    inv_batch = 1.0 / dp_size

    def device_step(tokens, grad_out, norm_attn, w_query, w_key, w_value, w_out, norm_mlp, w_gate, w_up, w_down):
        x = tokens[0]
        dy = grad_out[0]
        n_local, dim = x.shape
        n_seq = n_local * sp_size
        q_width = w_query.shape[1] // sp_size
        k_width = w_key.shape[1] // sp_size
        ff_local = w_gate.shape[1] // mlp_size
        rows = dim // dp_size
        attn_blk = min(512, n_seq // 2)

        def to_heads(stacked):
            return lax.all_to_all(stacked, seq_axes, 0, 0, tiled=True)

        def gather(local, axes):
            return lax.all_gather(local, axes, axis=0, tiled=True)

        normed, unit_attn, inv_attn = norm_fwd(x, norm_attn)
        dy_full = gather(dy, mlp_axes)
        normed_full, qkv = gather_qkv(normed, w_query, w_key, w_value, sp_size, 3)
        _, lse, attn_tok = attn_fwd(qkv, sp_size // 2, 4)
        w_out_heads = w_out.reshape(sp_size, q_width, dim)
        projected = jnp.einsum("jte,jed->td", attn_tok, w_out_heads, preferred_element_type=F32)
        hidden = (x.astype(F32) + projected).astype(BF16)
        normed_mlp, unit_mlp, inv_mlp = norm_fwd(hidden, norm_mlp)
        m_full = gather(normed_mlp, mlp_axes)

        grad_m = mlp_grad_input(normed_mlp, dy, w_gate, w_up, w_down, min(512, w_gate.shape[1]))
        grad_hid_norm, g_norm_mlp = norm_bwd(grad_m, unit_mlp, inv_mlp, norm_mlp)
        grad_hidden = (dy.astype(F32) + grad_hid_norm).astype(BF16)
        grad_hidden_y = gather(grad_hidden, mlp_axes)
        attn_y = lax.all_to_all(attn_tok, mlp_axes, 0, 0, tiled=True).reshape(n_seq, q_width)

        g_mlp = mlp_ring(m_full, dy_full, w_gate, w_up, w_down, ff_local, inv_batch, "z", "x", side, mlp_axes, 1)
        g_mlp, late_hidden = lax.optimization_barrier((g_mlp, grad_hidden))
        g_mlp = gather(g_mlp, ("z", "x", "y", "c"))

        grad_attn = to_head_groups(late_hidden, w_out, sp_size)
        grad_attn = to_heads(grad_attn).reshape(n_seq, q_width)
        g_out = outer(grad_hidden_y, attn_y).reshape(mlp_outer, rows, q_width)
        g_out = ring_reduce(g_out, inv_batch, 1, "z", "x", 5)

        gqkv = attn_bwd(qkv, grad_attn, lse, attn_blk)
        gqkv_tok = to_heads(gqkv.reshape(sp_size, n_local, q_width + 2 * k_width))
        grad_normed = from_head_groups(gqkv_tok, w_query, w_key, w_value)
        grad_tok_norm, g_norm_attn = norm_bwd(grad_normed, unit_attn, inv_attn, norm_attn)
        grad_tokens = (grad_hidden.astype(F32) + grad_tok_norm).astype(BF16)

        g_attn = outer(normed_full, gqkv).reshape(dp_size, rows, q_width + 2 * k_width)
        gains = jnp.stack([g_norm_attn.reshape(dp_size, rows), g_norm_mlp.reshape(dp_size, rows)], axis=1)
        gains = jnp.pad(gains.astype(BF16), ((0, 0), (0, rows - 2), (0, 0)))
        g_attn = ring_reduce(jnp.concatenate([g_attn, gains], axis=2), inv_batch, 2, "z", "y", 2)
        gain_at = q_width + 2 * k_width
        gains = jnp.pad(g_attn[:8, gain_at:], ((0, 0), (0, 2 * (q_width + k_width) - rows)))
        g_attn = jnp.concatenate([jnp.concatenate([g_attn[:, :gain_at], g_out], axis=1), gains], axis=0)
        g_attn = gather(g_attn, ("z", "y", "x", "c"))

        g_gate, g_up, g_down = spread_mlp(g_mlp, mlp_outer, mlp_size, ff_local)
        g_query, g_key, g_value, g_out, gains = spread_attn(g_attn, side, dp_size // side, sp_size, q_width, k_width)
        gains = gains.reshape(dp_size, 8, rows)
        return (
            grad_tokens[None],
            gains[:, 0].reshape(dim),
            g_query,
            g_key,
            g_value,
            g_out,
            gains[:, 1].reshape(dim),
            g_gate,
            g_up,
            g_down,
        )

    return jax.shard_map(device_step, mesh=grid, in_specs=(seq_spec, seq_spec) + (P(),) * 9, out_specs=(seq_spec,) + (P(),) * 9, check_vma=False)
```
